256 devices in a mesh: section: 2 (over core), expert: 128 (over x, z, y).
Axes of the slice: x: 4, y: 4, z: 8, core: 2. Of those that a mesh axis runs over, the one named last changes fastest.
Arguments:
- tokens: bfloat16 [2, 8192, 2048], P(None, 'expert'), may hold values from -6 to 6
- norm_gain: float32 [2, 2048], P('section'), may hold values from 0.5 to 2
- gate_weight: bfloat16 [2, 128, 2048, 768], P('section', 'expert'), may hold values from -0.125 to 0.125
- up_weight: bfloat16 [2, 128, 2048, 768], P('section', 'expert'), may hold values from -0.125 to 0.125
- down_weight: bfloat16 [2, 128, 768, 2048], P('section', 'expert'), may hold values from -0.21875 to 0.21875
- expert_place: int32 [2, 128], P('section'), may hold values from 0 to 127, each once within a row
- expert_ids: int32 [2, 2, 8192, 8], P('section', None, 'expert'), may hold values from 0 to 127, all different within a row; in each aligned block of 64 rows (0 to 63, 64 to 127, ..., all dimensions but the last counted through in order) at most 5 rows name the same one
- route_weights: float32 [2, 2, 8192, 8], P('section', None, 'expert'), may hold values from 0.05 to 0.4
Outputs:
- final_states: bfloat16 [2, 8192, 2048], P(None, 'expert')
The draws below stay inside these ranges and needn't reach their ends.
Inputs may be any that keep to these rules, and one draw needn't show every extreme that they name: `expert_ids`: each row names 8 different experts. In each aligned block of 64 rows (one device's tokens of one micro-batch in one layer) no expert is named by more than 5 rows, a bound that some block reaches. `expert_place`: each layer's row names every index along expert once.
All inputs are finite; a program needn't handle non-finite values.
Results may differ from the reference program's by a relative error of at most 0.013.
Values may be sent and summed in bfloat16 or wider, within the bound.
No kernel may reach another device: no remote copies, remote signals or barrier semaphores. Data moves between devices by JAX's collectives and lax.ppermute only.
A program may use at most 128 MiB of HBM per device.

```python
import math
import jax
import jax.numpy as jnp
import numpy as np
from jax import lax

D = 2048
FFE = 768
TOPK = 8
MB = 2
TOK_DEV = 64
EXPERTS = 128
LAYERS = 2
TOKENS = 8192
CAP = 5
N_EXPERT = 128


def level_of(stream_key, dims, split, smallest, top_value):
    factor_of = 1.0
    for axis_at, parts in split:
        draws = jax.random.uniform(jax.random.fold_in(jax.random.fold_in(stream_key, 6), axis_at), (parts,), jnp.float32, smallest / len(split), top_value / len(split))
        factor_of = factor_of * jnp.repeat(jnp.exp(draws), dims[axis_at] // parts).reshape((-1,) + (1,) * (len(dims) - 1 - axis_at))
    return factor_of


def deal_out(own_key, own, number, rows, number_of, top, reach, lean):
    order = jax.random.permutation(own_key, number_of)
    crowded, common = portions_of(number_of, rows * top, reach, lean, True), portions_of(number_of, rows * top, reach, lean, False)
    places = jnp.arange(number_of)

    def named(lengths, rotation):
        used = int((lengths > 0).sum())
        fixed = max(1, used // 4)
        moved = fixed + (places - fixed + rotation * (used - fixed)) % max(1, number_of - fixed)
        return jnp.zeros((number_of,), jnp.int32).at[order[jnp.where(places < fixed, places, moved)]].set(jnp.asarray(lengths, jnp.int32))

    lengths = jnp.where(number % 4 == 0, named(crowded, number // 4), named(common, number - number // 4 - 1))
    mixed = jax.random.permutation(jax.random.fold_in(own, 3), number_of)
    source_of, sink = mixed[0:number_of // 2 * 2:2], mixed[1:number_of // 2 * 2:2]
    room = jnp.minimum(lengths[source_of] - 1, reach - lengths[sink]) // 2
    room = jnp.where((source_of == order[0]) | (sink == order[0]) | (lengths[sink] == 0), 0, jnp.maximum(room, 0))
    moved = jax.random.randint(jax.random.fold_in(own, 4), (number_of // 2,), 0, 1 << 20) % (room + 1)
    lengths = lengths.at[source_of].add(-moved).at[sink].add(moved)
    items = jnp.searchsorted(jnp.cumsum(lengths), jnp.arange(rows * top), side="right").astype(jnp.int32)
    table = items.reshape(top, rows).T
    table = table[jax.random.permutation(jax.random.fold_in(own, 1), rows)]
    rotation = jax.random.randint(jax.random.fold_in(own, 2), (rows, 1), 0, top)
    return jnp.take_along_axis(table, (jnp.arange(top)[None, :] + rotation) % top, axis=1)


def portions_of(number_of, total, limit, skew, full):
    weights = [(1 << 20) // math.isqrt(grade ** skew) + 1 for grade in range(1, number_of + 1)]
    largest = limit if full else min(limit, max(-(-total // number_of), total * weights[0] // sum(weights)))
    least = 1 if total - largest >= number_of - 1 else 0
    counts, spare = [largest] + [least] * (number_of - 1), total - largest - least * (number_of - 1)
    while spare > 0:
        candidates = [i for i in range(1, number_of) if counts[i] < largest] or [i for i in range(1, number_of) if counts[i] < limit]
        pool, left = sum([weights[i] for i in candidates]), spare
        for i in candidates:
            more = min(limit - counts[i], max(1, left * weights[i] // pool), spare)
            counts[i] = counts[i] + more
            spare = spare - more
    return np.array(counts)


def bell_draw(rng, extent, deviation, most, cuts=(), held_as=jnp.bfloat16):
    entries = deviation * jax.random.normal(rng, extent, jnp.float32)
    if cuts:
        entries = entries * level_of(rng, extent, cuts, -0.22, 0.18)
    return jnp.clip(entries, -most, most).astype(held_as)


def setup_inputs(seed: int = 0) -> dict:
    splits = jax.random.split(jax.random.key(seed), 9)
    tokens = bell_draw(splits[0], (MB, TOKENS, D), 1.0, 6.0, ((1, 128),))
    norm_gain = jnp.clip(jnp.exp(math.log(2.0) - 1.3862944 * jax.random.uniform(splits[1], (LAYERS, D), jnp.float32) ** level_of(splits[1], (LAYERS, D), ((0, 2),), -0.2, 0.2)), 0.5, 2.0)
    gate_weight = bell_draw(splits[2], (LAYERS, EXPERTS, D, FFE), D ** -0.5, 0.125, ((0, 2), (1, 128)))
    up_weight = bell_draw(splits[3], (LAYERS, EXPERTS, D, FFE), D ** -0.5, 0.125, ((0, 2), (1, 128)))
    down_weight = bell_draw(splits[4], (LAYERS, EXPERTS, FFE, D), FFE ** -0.5, 0.21875, ((0, 2), (1, 128)))
    expert_place = jax.vmap(lambda own: jax.random.permutation(own, EXPERTS))(jax.random.split(splits[5], LAYERS)).reshape((LAYERS, EXPERTS)).astype(jnp.int32)
    expert_ids_keys = jax.random.split(jax.random.fold_in(splits[6], 1), LAYERS * MB * TOKENS // TOK_DEV)
    expert_ids_turns = jax.random.permutation(jax.random.fold_in(splits[6], 3), LAYERS * MB * TOKENS // TOK_DEV)
    expert_ids = jax.vmap(lambda own, number: deal_out(jax.random.fold_in(splits[6], 2), own, number, TOK_DEV, EXPERTS, TOPK, CAP, 2))(expert_ids_keys, expert_ids_turns).reshape((LAYERS, MB, TOKENS, TOPK))
    route_weights = jnp.clip(0.05 + 0.35 * jax.random.uniform(splits[7], (LAYERS, MB, TOKENS, TOPK), jnp.float32) ** level_of(splits[7], (LAYERS, MB, TOKENS, TOPK), ((0, 2), (2, 128)), -0.2, 0.2), 0.05, 0.4)
    return dict(tokens=tokens, norm_gain=norm_gain, gate_weight=gate_weight, up_weight=up_weight, down_weight=down_weight, expert_place=expert_place, expert_ids=expert_ids, route_weights=route_weights)


EPSILON = 1e-06

def normalize(values, gain_row):
    widened = values.astype(jnp.float32)
    inverse_rms = lax.rsqrt(lax.optimization_barrier(jnp.mean(widened * widened, axis=-1, keepdims=True)) + EPSILON)
    return (widened * inverse_rms * gain_row[None, :]).astype(jnp.bfloat16)

def slot_positions(block_ids):
    onehot = (block_ids[..., None] == jnp.arange(EXPERTS, dtype=jnp.int32)).astype(jnp.int32)
    before = jnp.cumsum(onehot, axis=1) - onehot
    return lax.optimization_barrier(jnp.sum(before * onehot, axis=-1)).astype(jnp.int32)

def moe_layer(hidden, gain_row, gate_matrix, up_matrix, down_matrix, holder_table, chosen, weights):
    normed = normalize(hidden, gain_row)
    block_ids = chosen.reshape(N_EXPERT, TOK_DEV * TOPK)
    position = slot_positions(block_ids).reshape(-1)
    flat_ids = chosen.reshape(-1).astype(jnp.int32)
    entry_index = jnp.arange(TOKENS * TOPK, dtype=jnp.int32)
    source = entry_index // (TOK_DEV * TOPK)
    target = (flat_ids * N_EXPERT + source) * CAP + position
    token_row = entry_index // TOPK
    buffer = jnp.zeros((EXPERTS * N_EXPERT * CAP, D), jnp.bfloat16).at[target].set(normed[token_row])
    buffer = buffer.reshape(EXPERTS, N_EXPERT * CAP, D)

    def run_expert(expert):
        holder = holder_table[expert]
        row_block = buffer[expert]
        gate_part = jnp.dot(row_block, gate_matrix[holder], preferred_element_type=jnp.float32)
        up_part = jnp.dot(row_block, up_matrix[holder], preferred_element_type=jnp.float32)
        hidden_units = (jax.nn.silu(gate_part) * up_part).astype(jnp.bfloat16)
        return jnp.dot(hidden_units, down_matrix[holder], preferred_element_type=jnp.float32).astype(jnp.bfloat16)
    outputs = lax.map(run_expert, jnp.arange(EXPERTS, dtype=jnp.int32)).reshape(-1, D)
    picked = outputs[target].astype(jnp.float32).reshape(TOKENS, TOPK, D)
    mixture = jnp.einsum('tk,tkd->td', weights.astype(jnp.float32), picked)
    return (hidden.astype(jnp.float32) + mixture).astype(jnp.bfloat16)

def reference(tokens, norm_gain, gate_weight, up_weight, down_weight, expert_place, expert_ids, route_weights):
    finals = []
    for micro_index in range(MB):
        hidden = tokens[micro_index]
        for layer_index in range(LAYERS):
            hidden = moe_layer(hidden, norm_gain[layer_index], gate_weight[layer_index], up_weight[layer_index], down_weight[layer_index], expert_place[layer_index], expert_ids[layer_index, micro_index], route_weights[layer_index, micro_index])
        finals.append(hidden)
    return jnp.stack(finals)
```

```python
import functools

import jax
import jax.numpy as jnp
from jax import lax
from jax.experimental import pallas as pl
from jax.experimental.pallas import tpu as pltpu
from jax.sharding import Mesh, PartitionSpec as P

EPSILON = 1e-06
LINE = 8
CAP = 5
BF = jnp.bfloat16
F32 = jnp.float32
VMEM = pltpu.MemorySpace.VMEM
SMEM = pltpu.MemorySpace.SMEM
HBM = pl.ANY


def vmem():
    return pl.BlockSpec(memory_space=VMEM)


def smem():
    return pl.BlockSpec(memory_space=SMEM)


def params(mib):
    return pltpu.CompilerParams(vmem_limit_bytes=mib << 20)


def shift(array, axis, by, size):
    return lax.ppermute(array, axis, [(i, (i + by) % size) for i in range(size)])


def normalized(hidden, gain):
    inverse = lax.rsqrt(jnp.mean(hidden * hidden, axis=-1, keepdims=True) + EPSILON)
    return (hidden * inverse * gain).astype(BF)


def routing_rows(ids, weights, place_column):
    tok = ids.shape[1]
    experts = lax.broadcasted_iota(jnp.int32, (128, tok), 0)
    hits = [(ids[k : k + 1, :] == experts).astype(F32) for k in range(8)]
    has = functools.reduce(jnp.add, hits)
    earlier = (
        lax.broadcasted_iota(jnp.int32, (tok, tok), 0) < lax.broadcasted_iota(jnp.int32, (tok, tok), 1)
    ).astype(F32)
    before = jnp.dot(has.astype(BF), earlier.astype(BF), preferred_element_type=F32)
    holders = [jnp.sum(h * place_column, axis=0, keepdims=True) for h in hits]
    positions = [jnp.sum(h * before, axis=0, keepdims=True) for h in hits]
    return jnp.concatenate(holders + positions + [weights, jnp.zeros_like(weights)], axis=0)


def prepare_kernel(sec, tok, gain_a, gain_b, place_a, place_b, ids_a, ids_b, wts_a, wts_b, low, high):
    s = sec[0]
    mine = s == 0
    hidden = tok[s].astype(F32)
    gain = jnp.where(mine, gain_a[...], gain_b[...])
    normed = normalized(hidden, gain)
    half = normed.shape[1] // 2
    low[...] = normed[:, :half]
    high[:, :half] = normed[:, half:]
    rows = []
    for first in (True, False):
        own = mine if first else jnp.logical_not(mine)
        ids = jnp.where(own, ids_a[s], ids_b[s])
        wts = jnp.where(own, wts_a[s], wts_b[s])
        place = jnp.where(own, place_a[...], place_b[...])
        rows.append(routing_rows(ids, wts, place.astype(F32)))
    table = jnp.concatenate(rows, axis=0)
    table = jnp.concatenate([table, jnp.zeros_like(table)], axis=1)
    table = jnp.concatenate([table, jnp.zeros_like(table)], axis=0)
    high[:, half:] = table.T[: low.shape[0], :].astype(BF)


def gather_body(zi, metas, blocks_low, blocks_high, layer, out, whole, emit):
    tok = 64
    half = whole.shape[1] // 2
    for i in range(LINE):
        whole[i * tok : (i + 1) * tok, :half] = blocks_low[i][...]
        whole[i * tok : (i + 1) * tok, half:] = blocks_high[i][:, :half]
    meta = metas()
    if emit is not None:
        emit[...] = meta
    rows = meta.astype(F32).T[layer * 32 : layer * 32 + 16, :]
    holder = rows[:8].astype(jnp.int32)
    rank = rows[8:].astype(jnp.int32)
    block = lax.broadcasted_iota(jnp.int32, holder.shape, 1) // tok
    place = ((holder // 32) * 4 + holder % 4) * (LINE * CAP) + block * CAP + rank
    slot = jnp.where((holder // 4) % LINE == zi, place, -1)
    total = out.shape[0]
    lanes = LINE * tok
    step = 128
    for r in range(0, total, step):
        index = lax.broadcasted_iota(jnp.int32, (step, lanes), 0) + r
        hit = index == slot[0:1, :]
        for k in range(1, 8):
            hit = jnp.logical_or(hit, index == slot[k : k + 1, :])
        pick = jnp.where(hit, 1.0, 0.0).astype(BF)
        out[r : r + step, :] = jnp.dot(pick, whole[...], preferred_element_type=F32).astype(BF)


def gather_first_kernel(zi, *refs):
    low, high = refs[:LINE], refs[LINE : 2 * LINE]
    out, emit, whole = refs[2 * LINE :]
    half = low[0].shape[1]
    metas = lambda: jnp.concatenate([h[:, half:] for h in high], axis=0)
    gather_body(zi[0], metas, low, high, 0, out, whole, emit)


def gather_later_kernel(zi, meta, *refs):
    low, high = refs[:LINE], refs[LINE : 2 * LINE]
    out, whole = refs[2 * LINE :]
    gather_body(zi[0], lambda: meta[...], low, high, 1, out, whole, None)


def ffn_kernel(layer, sec, rows, ga, ua, da, gb, ub, db, out, wg, wu, wd, gate, up, sems):
    own = sec[0] == layer
    half = wg.shape[0] // 2
    pieces = []
    for a, b, dst, lo, size in (
        (ga, gb, wg, 0, half),
        (ua, ub, wu, 0, half),
        (ga, gb, wg, half, half),
        (ua, ub, wu, half, half),
        (da, db, wd, 0, wd.shape[0]),
    ):
        part = pl.ds(lo, size)
        n = len(pieces)
        pieces.append(
            (
                pltpu.make_async_copy(a.at[part], dst.at[part], sems.at[n]),
                pltpu.make_async_copy(b.at[part], dst.at[part], sems.at[n]),
            )
        )

    @pl.when(own)
    def _():
        for mine, _ in pieces:
            mine.start()

    @pl.when(jnp.logical_not(own))
    def _():
        for _, theirs in pieces:
            theirs.start()

    dot = functools.partial(jnp.dot, preferred_element_type=F32)
    pieces[0][0].wait()
    gate[...] = dot(rows[:, :half], wg[:half])
    pieces[1][0].wait()
    up[...] = dot(rows[:, :half], wu[:half])
    pieces[2][0].wait()
    gate[...] += dot(rows[:, half:], wg[half:])
    pieces[3][0].wait()
    v = gate[...]
    hidden = (v / (1.0 + jnp.exp(-v)) * (up[...] + dot(rows[:, half:], wu[half:]))).astype(BF)
    pieces[4][0].wait()
    out[...] = dot(hidden, wd[...]).astype(BF)


def combine_kernel(layer, zi, meta, rows, *outs):
    tok = 64
    half = rows.shape[1] // 2
    table = meta[:, layer * 32 : layer * 32 + 24].astype(F32)
    holder = table[:, :8].astype(jnp.int32)
    rank = table[:, 8:16].astype(jnp.int32)
    block = lax.broadcasted_iota(jnp.int32, holder.shape, 0) // tok
    place = ((holder // 32) * 4 + holder % 4) * (LINE * CAP) + block * CAP + rank
    slot = jnp.where((holder // 4) % LINE == zi[0], place, -1)
    total = rows.shape[0]
    for i in range(0, LINE, 2):
        part = slice(i * tok, (i + 2) * tok)
        index = lax.broadcasted_iota(jnp.int32, (2 * tok, total), 1)
        mix = jnp.zeros((2 * tok, total), F32)
        for k in range(8):
            mix = jnp.where(index == slot[part, k : k + 1], table[part, 16 + k : 17 + k], mix)
        mix = mix.astype(BF)
        for c in range(2):
            total_rows = jnp.dot(mix, rows[:, c * half : (c + 1) * half], preferred_element_type=F32)
            for b in range(2):
                outs[2 * (i + b) + c][...] = total_rows[b * tok : (b + 1) * tok].astype(BF)


def middle_kernel(sec, tok, gain_a, gain_b, *refs):
    f0, f1, b0, b1, p0, p1, kept, low, high = refs
    s = sec[0]
    hidden = tok[s].astype(F32)
    half = hidden.shape[1] // 2
    add = lambda x, y, z: x[...].astype(F32) + y[...].astype(F32) + z[...].astype(F32)
    hidden = hidden + jnp.concatenate([add(p0, f0, b0), add(p1, f1, b1)], axis=1)
    hidden = hidden.astype(BF)
    kept[...] = hidden
    gain = jnp.where(s == 0, gain_b[...], gain_a[...])
    normed = normalized(hidden.astype(F32), gain)
    low[...] = normed[:, :half]
    high[...] = normed[:, half:]


def last_kernel(hidden, f0, f1, b0, b1, p0, p1, out):
    half = f0.shape[1]
    add = lambda x, y, z: x[...].astype(F32) + y[...].astype(F32) + z[...].astype(F32)
    out[:, :half] = (hidden[:, :half].astype(F32) + add(p0, f0, b0)).astype(BF)
    out[:, half:] = (hidden[:, half:].astype(F32) + add(p1, f1, b1)).astype(BF)


ORDER = (0, -1, 1, -2, 2, -3, 3, 4)


def line_gather(low, high):
    held = {0: (low, high)}
    ahead, behind = (low, high), (low, high)
    for step in (1, 2, 3):
        behind = tuple(shift(p, "z", 1, LINE) for p in behind)
        ahead = tuple(shift(p, "z", -1, LINE) for p in ahead)
        held[-step], held[step] = behind, ahead
    held[4] = (shift(behind[0], "z", 1, LINE), shift(ahead[1], "z", -1, LINE))
    return [held[o][0] for o in ORDER], [held[o][1] for o in ORDER]


def line_scatter(parts):
    low = {o: parts[2 * i] for i, o in enumerate(ORDER)}
    high = {o: parts[2 * i + 1] for i, o in enumerate(ORDER)}
    up = lambda p: shift(p, "z", 1, LINE)
    down = lambda p: shift(p, "z", -1, LINE)
    f0, b1 = up(low[4]), down(high[4])
    f0, b1 = up(low[3] + f0), down(high[-3] + b1)
    f1, b0 = up(high[3]), down(low[-3])
    for step in (2, 1):
        f0, f1 = up(low[step] + f0), up(high[step] + f1)
        b0, b1 = down(low[-step] + b0), down(high[-step] + b1)
    return f0, f1, b0, b1, low[0], high[0]


def plane_exchange(rows):
    parts = rows.reshape(16, rows.shape[0] // 16, rows.shape[1])
    return lax.all_to_all(parts, ("x", "y"), 0, 0, tiled=True).reshape(rows.shape)


def local(
    tokens, norm_gain, gate_weight, up_weight, down_weight, expert_place, expert_ids, route_weights
):
    section = lax.axis_index("section").astype(jnp.int32)[None]
    plane = lax.axis_index("z").astype(jnp.int32)[None]
    tok, width = tokens.shape[1], tokens.shape[2]
    half = width // 2
    slots = 16 * LINE * CAP
    ffe = gate_weight.shape[3]
    sds = jax.ShapeDtypeStruct

    swap = lambda v: shift(v, "section", 1, 2)
    ids = jnp.swapaxes(expert_ids[0], 1, 2)
    wts = jnp.swapaxes(route_weights[0], 1, 2)
    place = expert_place.reshape(128, 1)
    mats = (gate_weight[0, 0], up_weight[0, 0], down_weight[0, 0])
    gain_b, place_b, ids_b, wts_b = swap(norm_gain), swap(expert_place), swap(ids), swap(wts)
    place_b = place_b.reshape(128, 1)
    mats_b = tuple(swap(m) for m in mats)

    low, high = pl.pallas_call(
        prepare_kernel,
        out_shape=(sds((tok, half), BF), sds((tok, half + 128), BF)),
        in_specs=[smem()] + [vmem()] * 9,
        out_specs=(vmem(), vmem()),
        compiler_params=params(16),
        name="prepare",
    )(section, tokens, norm_gain, gain_b, place, place_b, ids, ids_b, wts, wts_b)

    def experts(rows, layer):
        return pl.pallas_call(
            functools.partial(ffn_kernel, layer),
            out_shape=sds((slots, width), BF),
            in_specs=[smem(), vmem()] + [pl.BlockSpec(memory_space=HBM)] * 6,
            out_specs=vmem(),
            scratch_shapes=[
                pltpu.VMEM((width, ffe), BF),
                pltpu.VMEM((width, ffe), BF),
                pltpu.VMEM((ffe, width), BF),
                pltpu.VMEM((slots, ffe), F32),
                pltpu.VMEM((slots, ffe), F32),
                pltpu.SemaphoreType.DMA((5,)),
            ],
            compiler_params=params(40),
            name="experts",
        )(section, rows, *mats, *mats_b)

    def combine(rows, meta, layer):
        return pl.pallas_call(
            functools.partial(combine_kernel, layer),
            out_shape=[sds((tok, half), BF)] * (2 * LINE),
            in_specs=[smem(), vmem(), vmem()],
            out_specs=[vmem()] * (2 * LINE),
            compiler_params=params(32),
            name="combine",
        )(plane, meta, rows)

    lows, highs = line_gather(low, high)
    outgoing, meta = pl.pallas_call(
        gather_first_kernel,
        out_shape=(sds((slots, width), BF), sds((LINE * tok, 128), BF)),
        in_specs=[smem()] + [vmem()] * (2 * LINE),
        out_specs=(vmem(), vmem()),
        scratch_shapes=[pltpu.VMEM((LINE * tok, width), BF)],
        compiler_params=params(32),
        name="spread",
    )(plane, *lows, *highs)
    returned = plane_exchange(experts(plane_exchange(outgoing), 0))
    sums = line_scatter(combine(returned, meta, 0))

    hidden, low, high = pl.pallas_call(
        middle_kernel,
        out_shape=(sds((tok, width), BF), sds((tok, half), BF), sds((tok, half), BF)),
        in_specs=[smem()] + [vmem()] * 9,
        out_specs=(vmem(), vmem(), vmem()),
        compiler_params=params(16),
        name="middle",
    )(section, tokens, norm_gain, gain_b, *sums)

    lows, highs = line_gather(low, high)
    outgoing = pl.pallas_call(
        gather_later_kernel,
        out_shape=sds((slots, width), BF),
        in_specs=[smem()] + [vmem()] * (2 * LINE + 1),
        out_specs=vmem(),
        scratch_shapes=[pltpu.VMEM((LINE * tok, width), BF)],
        compiler_params=params(32),
        name="spread_later",
    )(plane, meta, *lows, *highs)
    returned = plane_exchange(experts(plane_exchange(outgoing), 1))
    sums = line_scatter(combine(returned, meta, 1))

    final = pl.pallas_call(
        last_kernel,
        out_shape=sds((tok, width), BF),
        in_specs=[vmem()] * 7,
        out_specs=vmem(),
        compiler_params=params(16),
        name="last",
    )(hidden, *sums)
    theirs = swap(final)
    mine_first = section[0] == 0
    return jnp.stack([jnp.where(mine_first, final, theirs), jnp.where(mine_first, theirs, final)])


def solution(mesh):
    fine = Mesh(mesh.devices.reshape(2, 4, 8, 4), ("section", "x", "z", "y"))
    line = ("x", "z", "y")
    in_specs = (
        P(None, line, None),
        P("section", None),
        P("section", line, None, None),
        P("section", line, None, None),
        P("section", line, None, None),
        P("section", None),
        P("section", None, line, None),
        P("section", None, line, None),
    )
    return jax.shard_map(
        local, mesh=fine, in_specs=in_specs, out_specs=P(None, line, None), check_vma=False
    )
```

```python
import functools

import jax
import jax.numpy as jnp
from jax import lax
from jax.experimental import pallas as pl
from jax.experimental.pallas import tpu as pltpu
from jax.sharding import Mesh, PartitionSpec as P

EPSILON = 1e-06
LINE = 8
CAP = 5
BF = jnp.bfloat16
F32 = jnp.float32
VMEM = pltpu.MemorySpace.VMEM
SMEM = pltpu.MemorySpace.SMEM
HBM = pltpu.MemorySpace.HBM


def vmem():
    return pl.BlockSpec(memory_space=VMEM)


def smem():
    return pl.BlockSpec(memory_space=SMEM)


def params(mib):
    return pltpu.CompilerParams(vmem_limit_bytes=mib << 20)


def shift(array, axis, by, size):
    return lax.ppermute(array, axis, [(i, (i + by) % size) for i in range(size)])


def normalized(hidden, gain):
    inverse = lax.rsqrt(jnp.mean(hidden * hidden, axis=-1, keepdims=True) + EPSILON)
    return (hidden * inverse * gain).astype(BF)


def routing_rows(ids, weights, place_row):
    tok = ids.shape[1]
    experts = lax.broadcasted_iota(jnp.int32, (128, tok), 0).astype(F32)
    hits = [(ids[k : k + 1, :] == experts).astype(F32) for k in range(8)]
    has = functools.reduce(jnp.add, hits)
    earlier = (
        lax.broadcasted_iota(jnp.int32, (tok, tok), 0) < lax.broadcasted_iota(jnp.int32, (tok, tok), 1)
    ).astype(F32)
    dot = functools.partial(jnp.dot, preferred_element_type=F32)
    before = dot(has.astype(BF), earlier.astype(BF))
    places = jnp.broadcast_to(place_row, (8, 128)).astype(BF)
    holders = [dot(places, h.astype(BF))[:1] for h in hits]
    positions = [jnp.sum(h * before, axis=0, keepdims=True) for h in hits]
    return jnp.concatenate(holders + positions + [weights, jnp.zeros_like(weights)], axis=0)


def pack_kernel(sec, tok, gain, place, ids, wts, table, hidden, gain_v, place_v, ids_v, wts_v, sems):
    copies = [
        pltpu.make_async_copy(gain, gain_v, sems.at[0]),
        pltpu.make_async_copy(place, place_v, sems.at[1]),
        pltpu.make_async_copy(ids, ids_v, sems.at[2]),
        pltpu.make_async_copy(wts, wts_v, sems.at[3]),
        pltpu.make_async_copy(tok.at[sec[0]], hidden, sems.at[4]),
    ]
    for c in copies:
        c.start()
    table[...] = jnp.zeros(table.shape, F32)
    for c in copies[:4]:
        c.wait()
    for i in range(16):
        table[i : i + 1, :] = gain_v[:, 128 * i : 128 * (i + 1)]
    for m in range(2):
        table[16 + 8 * m : 24 + 8 * m, :64] = ids_v[m].astype(F32)
        table[32 + 8 * m : 40 + 8 * m, :64] = wts_v[m]
    table[48:49, :] = place_v[...].astype(F32)
    copies[4].wait()


def gain_of(table):
    return jnp.concatenate([table[i : i + 1, :] for i in range(16)], axis=1)


def prepare_kernel(sec, hidden, mine, theirs, payload):
    s = sec[0]
    first = jnp.where(s == 0, mine[...], theirs[...])
    second = jnp.where(s == 0, theirs[...], mine[...])
    width = hidden.shape[1]
    payload[:, :width] = normalized(hidden[...].astype(F32), gain_of(first))
    rows = []
    for table in (first, second):
        ids = jnp.where(s == 0, table[16:24, :64], table[24:32, :64])
        wts = jnp.where(s == 0, table[32:40, :64], table[40:48, :64])
        rows.append(routing_rows(ids, wts, table[48:49, :]))
    table = jnp.concatenate(rows, axis=0)
    table = jnp.concatenate([table, jnp.zeros_like(table)], axis=1)
    table = jnp.concatenate([table, jnp.zeros_like(table)], axis=0)
    payload[:, width:] = table.T[: hidden.shape[0], :].astype(BF)


def slot_of(holder, rank, block, zi):
    place = ((holder // 32) * 4 + holder % 4) * (LINE * CAP) + block * CAP + rank
    return jnp.where((holder // 4) % LINE == zi, place, -1)


def gather_body(zi, meta, blocks, layer, out, whole, pick, codes):
    tok = 64
    width = whole.shape[1]
    for i in range(LINE):
        whole[i * tok : (i + 1) * tok, :] = blocks[i][:, :width]
    rows = meta.astype(F32).T[layer * 32 : layer * 32 + 16, :]
    holder = rows[:8].astype(jnp.int32)
    block = lax.broadcasted_iota(jnp.int32, holder.shape, 1) // tok
    codes[...] = slot_of(holder, rows[8:].astype(jnp.int32), block, zi)
    step = 128

    def build(r, carry):
        index = lax.broadcasted_iota(jnp.int32, (step, LINE * tok), 0) + r * step
        hit = index == codes[0:1, :]
        for k in range(1, 8):
            hit = jnp.logical_or(hit, index == codes[k : k + 1, :])
        pick[pl.ds(pl.multiple_of(r * step, step), step), :] = jnp.where(hit, 1.0, 0.0).astype(BF)
        return carry

    lax.fori_loop(0, out.shape[0] // step, build, 0)

    def spread(n, carry):
        part = pl.ds(pl.multiple_of(n * 512, 512), 512)
        out[:, part] = jnp.dot(pick[...], whole[:, part], preferred_element_type=F32).astype(BF)
        return carry

    lax.fori_loop(0, width // 512, spread, 0)


def gather_first_kernel(zi, *refs):
    blocks = refs[:LINE]
    out, emit, whole, pick, codes = refs[LINE:]
    width = whole.shape[1]
    for i in range(LINE):
        emit[i * 64 : (i + 1) * 64, :] = blocks[i][:, width:]
    gather_body(zi[0], emit[...], blocks, 0, out, whole, pick, codes)


def gather_later_kernel(zi, meta, *refs):
    blocks = refs[:LINE]
    out, whole, pick, codes = refs[LINE:]
    gather_body(zi[0], meta[...], blocks, 1, out, whole, pick, codes)


PIECES = 4


def ffn_kernel(layer, sec, rows, ga, ua, da, gb, ub, db, out, wg, wu, wd, gate, up, sems):
    own = sec[0] == layer
    size = wg.shape[0] // PIECES

    def copies(g, u, d):
        found = []
        for k in range(PIECES):
            part = pl.ds(k * size, size)
            found.append(pltpu.make_async_copy(g.at[part], wg.at[part], sems.at[0, k]))
            found.append(pltpu.make_async_copy(u.at[part], wu.at[part], sems.at[1, k]))
        return found + [pltpu.make_async_copy(d, wd, sems.at[0, PIECES])]

    @pl.when(own)
    def _():
        for c in copies(ga, ua, da):
            c.start()

    @pl.when(jnp.logical_not(own))
    def _():
        for c in copies(gb, ub, db):
            c.start()

    dot = functools.partial(jnp.dot, preferred_element_type=F32)
    gate[...] = jnp.zeros(gate.shape, F32)
    up[...] = jnp.zeros(up.shape, F32)

    def project(k, carry):
        part = pl.ds(pl.multiple_of(k * size, size), size)
        pltpu.make_async_copy(ga.at[part], wg.at[part], sems.at[0, k]).wait()
        gate[...] += dot(rows[:, part], wg[part, :])
        pltpu.make_async_copy(ua.at[part], wu.at[part], sems.at[1, k]).wait()
        up[...] += dot(rows[:, part], wu[part, :])
        return carry

    lax.fori_loop(0, PIECES, project, 0)
    v = gate[...]
    hidden = (v / (1.0 + jnp.exp(-v)) * up[...]).astype(BF)
    pltpu.make_async_copy(da, wd, sems.at[0, PIECES]).wait()

    def deliver(n, carry):
        part = pl.ds(pl.multiple_of(n * 512, 512), 512)
        out[:, part] = dot(hidden, wd[:, part]).astype(BF)
        return carry

    lax.fori_loop(0, out.shape[1] // 512, deliver, 0)


def combine_kernel(layer, zi, meta, rows, *refs):
    outs, mix = refs[:LINE], refs[LINE]
    tok = 64
    total = rows.shape[0]
    step = 128

    def weigh(i, carry):
        table = meta[pl.ds(pl.multiple_of(i * step, step), step), :].astype(F32)
        table = table[:, layer * 32 : layer * 32 + 24]
        holder = table[:, :8].astype(jnp.int32)
        block = (lax.broadcasted_iota(jnp.int32, holder.shape, 0) + i * step) // tok
        slot = slot_of(holder, table[:, 8:16].astype(jnp.int32), block, zi[0])
        index = lax.broadcasted_iota(jnp.int32, (step, total), 1)
        found = jnp.zeros((step, total), F32)
        for k in range(8):
            found = jnp.where(index == slot[:, k : k + 1], table[:, 16 + k : 17 + k], found)
        mix[pl.ds(pl.multiple_of(i * step, step), step), :] = found.astype(BF)
        return carry

    lax.fori_loop(0, LINE * tok // step, weigh, 0)

    def add_up(n, carry):
        part = pl.ds(pl.multiple_of(n * 512, 512), 512)
        sums = jnp.dot(mix[...], rows[:, part], preferred_element_type=F32).astype(BF)
        for i in range(LINE):
            outs[i][:, part] = sums[i * tok : (i + 1) * tok]
        return carry

    lax.fori_loop(0, rows.shape[1] // 512, add_up, 0)


def with_sums(hidden, sums):
    return (hidden[...].astype(F32) + sum(x[...].astype(F32) for x in sums)).astype(BF)


def middle_kernel(sec, hidden, mine, theirs, f, b, p, kept, payload):
    updated = with_sums(hidden, (p, f, b))
    kept[...] = updated
    gain = gain_of(jnp.where(sec[0] == 0, theirs[:16, :], mine[:16, :]))
    payload[...] = normalized(updated.astype(F32), gain)


def last_kernel(hidden, f, b, p, out):
    out[...] = with_sums(hidden, (p, f, b))


ORDER = (0, -1, 1, -2, 2, -3, 3, 4)


def line_gather(payload):
    held = {0: payload}
    ahead = behind = payload
    for step in (1, 2, 3):
        behind = shift(behind, "z", 1, LINE)
        ahead = shift(ahead, "z", -1, LINE)
        held[-step], held[step] = behind, ahead
    held[4] = shift(behind, "z", 1, LINE)
    return [held[o] for o in ORDER]


def line_scatter(parts):
    part = dict(zip(ORDER, parts))
    up = lambda p: shift(p, "z", 1, LINE)
    down = lambda p: shift(p, "z", -1, LINE)
    f, b = up(part[4]), down(part[-3])
    f, b = up(part[3] + f), down(part[-2] + b)
    f, b = up(part[2] + f), down(part[-1] + b)
    return up(part[1] + f), b, part[0]


def plane_exchange(rows):
    parts = rows.reshape(16, rows.shape[0] // 16, rows.shape[1])
    return lax.all_to_all(parts, ("x", "y"), 0, 0, tiled=True).reshape(rows.shape)


def local(
    tokens, norm_gain, gate_weight, up_weight, down_weight, expert_place, expert_ids, route_weights
):
    section = lax.axis_index("section").astype(jnp.int32)[None]
    plane = lax.axis_index("z").astype(jnp.int32)[None]
    tok, width = tokens.shape[1], tokens.shape[2]
    slots = 16 * LINE * CAP
    lanes = LINE * tok
    ffe = gate_weight.shape[3]
    sds = jax.ShapeDtypeStruct
    anywhere = pl.BlockSpec(memory_space=HBM)

    swap = lambda v: shift(v, "section", 1, 2)
    ids = jnp.swapaxes(expert_ids[0], 1, 2)
    wts = jnp.swapaxes(route_weights[0], 1, 2)
    mine, start = pl.pallas_call(
        pack_kernel,
        out_shape=(sds((56, 128), F32), sds((tok, width), BF)),
        in_specs=[smem()] + [anywhere] * 5,
        out_specs=(vmem(), vmem()),
        scratch_shapes=[
            pltpu.VMEM((1, width), F32),
            pltpu.VMEM((1, 128), jnp.int32),
            pltpu.VMEM((2, 8, tok), jnp.int32),
            pltpu.VMEM((2, 8, tok), F32),
            pltpu.SemaphoreType.DMA((5,)),
        ],
        compiler_params=params(8),
        name="pack",
    )(section, *(pltpu.with_memory_space_constraint(v, HBM) for v in (tokens, norm_gain, expert_place, ids, wts)))
    theirs = swap(mine)

    payload = pl.pallas_call(
        prepare_kernel,
        out_shape=sds((tok, width + 128), BF),
        in_specs=[smem()] + [vmem()] * 3,
        out_specs=vmem(),
        compiler_params=params(16),
        name="prepare",
    )(section, start, mine, theirs)

    def experts(rows, layer, mats, mats_b):
        return pl.pallas_call(
            functools.partial(ffn_kernel, layer),
            out_shape=sds((slots, width), BF),
            in_specs=[smem(), vmem()] + [anywhere] * 3 + [pl.BlockSpec(memory_space=pl.ANY)] * 3,
            out_specs=vmem(),
            scratch_shapes=[
                pltpu.VMEM((width, ffe), BF),
                pltpu.VMEM((width, ffe), BF),
                pltpu.VMEM((ffe, width), BF),
                pltpu.VMEM((slots, ffe), F32),
                pltpu.VMEM((slots, ffe), F32),
                pltpu.SemaphoreType.DMA((2, PIECES + 1)),
            ],
            compiler_params=params(32),
            name="experts",
        )(section, rows, *mats, *mats_b)

    def combine(rows, meta, layer):
        return pl.pallas_call(
            functools.partial(combine_kernel, layer),
            out_shape=[sds((tok, width), BF)] * LINE,
            in_specs=[smem(), vmem(), vmem()],
            out_specs=[vmem()] * LINE,
            scratch_shapes=[pltpu.VMEM((lanes, slots), BF)],
            compiler_params=params(20),
            name="combine",
        )(plane, meta, rows)

    gather_scratch = [
        pltpu.VMEM((lanes, width), BF),
        pltpu.VMEM((slots, lanes), BF),
        pltpu.VMEM((8, lanes), jnp.int32),
    ]
    outgoing, meta = pl.pallas_call(
        gather_first_kernel,
        out_shape=(sds((slots, width), BF), sds((lanes, 128), BF)),
        in_specs=[smem()] + [vmem()] * LINE,
        out_specs=(vmem(), vmem()),
        scratch_shapes=gather_scratch,
        compiler_params=params(20),
        name="spread",
    )(plane, *line_gather(payload))

    mats = (gate_weight[0, 0], up_weight[0, 0], down_weight[0, 0])
    outgoing, mats = lax.optimization_barrier((outgoing, mats))
    mats_b = tuple(swap(m) for m in mats)
    mats = tuple(pltpu.with_memory_space_constraint(m, HBM) for m in mats)
    arrived = plane_exchange(outgoing)
    returned = plane_exchange(experts(arrived, 0, mats, mats_b))
    sums = line_scatter(combine(returned, meta, 0))

    hidden, payload = pl.pallas_call(
        middle_kernel,
        out_shape=(sds((tok, width), BF), sds((tok, width), BF)),
        in_specs=[smem()] + [vmem()] * 6,
        out_specs=(vmem(), vmem()),
        compiler_params=params(16),
        name="middle",
    )(section, start, mine, theirs, *sums)

    outgoing = pl.pallas_call(
        gather_later_kernel,
        out_shape=sds((slots, width), BF),
        in_specs=[smem()] + [vmem()] * (LINE + 1),
        out_specs=vmem(),
        scratch_shapes=gather_scratch,
        compiler_params=params(20),
        name="spread_later",
    )(plane, meta, *line_gather(payload))
    returned = plane_exchange(experts(plane_exchange(outgoing), 1, mats, mats_b))
    sums = line_scatter(combine(returned, meta, 1))

    final = pl.pallas_call(
        last_kernel,
        out_shape=sds((tok, width), BF),
        in_specs=[vmem()] * 4,
        out_specs=vmem(),
        compiler_params=params(16),
        name="last",
    )(hidden, *sums)
    theirs = swap(final)
    mine_first = section[0] == 0
    return jnp.stack([jnp.where(mine_first, final, theirs), jnp.where(mine_first, theirs, final)])


def solution(mesh):
    fine = Mesh(mesh.devices.reshape(2, 4, 8, 4), ("section", "x", "z", "y"))
    line = ("x", "z", "y")
    in_specs = (
        P(None, line, None),
        P("section", None),
        P("section", line, None, None),
        P("section", line, None, None),
        P("section", line, None, None),
        P("section", None),
        P("section", None, line, None),
        P("section", None, line, None),
    )
    return jax.shard_map(
        local, mesh=fine, in_specs=in_specs, out_specs=P(None, line, None), check_vma=False
    )
```

```python
import functools

import jax
import jax.numpy as jnp
from jax import lax
from jax.experimental import pallas as pl
from jax.experimental.pallas import tpu as pltpu
from jax.sharding import Mesh, PartitionSpec as P

EPSILON = 1e-06
LINE = 8
CAP = 5
BF = jnp.bfloat16
F32 = jnp.float32
VMEM = pltpu.MemorySpace.VMEM
SMEM = pltpu.MemorySpace.SMEM
HBM = pltpu.MemorySpace.HBM


def vmem():
    return pl.BlockSpec(memory_space=VMEM)


def smem():
    return pl.BlockSpec(memory_space=SMEM)


def params(mib):
    return pltpu.CompilerParams(vmem_limit_bytes=mib << 20)


def shift(array, axis, by, size):
    return lax.ppermute(array, axis, [(i, (i + by) % size) for i in range(size)])


def normalized(hidden, gain):
    inverse = lax.rsqrt(jnp.mean(hidden * hidden, axis=-1, keepdims=True) + EPSILON)
    return (hidden * inverse * gain).astype(BF)


def routing_rows(ids, weights, place_row):
    tok = ids.shape[1]
    experts = lax.broadcasted_iota(jnp.int32, (128, tok), 0).astype(F32)
    hits = [(ids[k : k + 1, :] == experts).astype(F32) for k in range(8)]
    has = functools.reduce(jnp.add, hits)
    earlier = (
        lax.broadcasted_iota(jnp.int32, (tok, tok), 0) < lax.broadcasted_iota(jnp.int32, (tok, tok), 1)
    ).astype(F32)
    dot = functools.partial(jnp.dot, preferred_element_type=F32)
    before = dot(has.astype(BF), earlier.astype(BF))
    places = jnp.broadcast_to(place_row, (8, 128)).astype(BF)
    holders = [dot(places, h.astype(BF))[:1] for h in hits]
    positions = [jnp.sum(h * before, axis=0, keepdims=True) for h in hits]
    return jnp.concatenate(holders + positions + [weights, jnp.zeros_like(weights)], axis=0)


def pack_kernel(sec, tok, gain, place, ids, wts, table, hidden, gain_v, place_v, ids_v, wts_v, sems):
    copies = [
        pltpu.make_async_copy(gain, gain_v, sems.at[0]),
        pltpu.make_async_copy(place, place_v, sems.at[1]),
        pltpu.make_async_copy(ids, ids_v, sems.at[2]),
        pltpu.make_async_copy(wts, wts_v, sems.at[3]),
        pltpu.make_async_copy(tok.at[sec[0]], hidden, sems.at[4]),
    ]
    for c in copies:
        c.start()
    table[...] = jnp.zeros(table.shape, F32)
    for c in copies[:4]:
        c.wait()
    for i in range(16):
        table[i : i + 1, :] = gain_v[:, 128 * i : 128 * (i + 1)]
    for m in range(2):
        table[16 + 8 * m : 24 + 8 * m, :64] = ids_v[m].astype(F32)
        table[32 + 8 * m : 40 + 8 * m, :64] = wts_v[m]
    table[48:49, :] = place_v[...].astype(F32)
    copies[4].wait()


def gain_of(table):
    return jnp.concatenate([table[i : i + 1, :] for i in range(16)], axis=1)


def prepare_kernel(sec, hidden, mine, theirs, low, high):
    s = sec[0]
    first = jnp.where(s == 0, mine[...], theirs[...])
    second = jnp.where(s == 0, theirs[...], mine[...])
    half = hidden.shape[1] // 2
    normed = normalized(hidden[...].astype(F32), gain_of(first))
    low[...] = normed[:, :half]
    high[:, :half] = normed[:, half:]
    rows = []
    for table in (first, second):
        ids = jnp.where(s == 0, table[16:24, :64], table[24:32, :64])
        wts = jnp.where(s == 0, table[32:40, :64], table[40:48, :64])
        rows.append(routing_rows(ids, wts, table[48:49, :]))
    table = jnp.concatenate(rows, axis=0)
    table = jnp.concatenate([table, jnp.zeros_like(table)], axis=1)
    table = jnp.concatenate([table, jnp.zeros_like(table)], axis=0)
    high[:, half:] = table.T[: hidden.shape[0], :].astype(BF)


def gather_body(zi, metas, blocks_low, blocks_high, layer, out, whole, emit):
    tok = 64
    half = whole.shape[1] // 2
    for i in range(LINE):
        whole[i * tok : (i + 1) * tok, :half] = blocks_low[i][...]
        whole[i * tok : (i + 1) * tok, half:] = blocks_high[i][:, :half]
    meta = metas()
    if emit is not None:
        emit[...] = meta
    rows = meta.astype(F32).T[layer * 32 : layer * 32 + 16, :]
    holder = rows[:8].astype(jnp.int32)
    rank = rows[8:].astype(jnp.int32)
    block = lax.broadcasted_iota(jnp.int32, holder.shape, 1) // tok
    place = ((holder // 32) * 4 + holder % 4) * (LINE * CAP) + block * CAP + rank
    slot = jnp.where((holder // 4) % LINE == zi, place, -1)
    total = out.shape[0]
    lanes = LINE * tok
    step = 128
    for r in range(0, total, step):
        index = lax.broadcasted_iota(jnp.int32, (step, lanes), 0) + r
        hit = index == slot[0:1, :]
        for k in range(1, 8):
            hit = jnp.logical_or(hit, index == slot[k : k + 1, :])
        pick = jnp.where(hit, 1.0, 0.0).astype(BF)
        out[r : r + step, :] = jnp.dot(pick, whole[...], preferred_element_type=F32).astype(BF)


def gather_first_kernel(zi, *refs):
    low, high = refs[:LINE], refs[LINE : 2 * LINE]
    out, emit, whole = refs[2 * LINE :]
    half = low[0].shape[1]
    metas = lambda: jnp.concatenate([h[:, half:] for h in high], axis=0)
    gather_body(zi[0], metas, low, high, 0, out, whole, emit)


def gather_later_kernel(zi, meta, *refs):
    low, high = refs[:LINE], refs[LINE : 2 * LINE]
    out, whole = refs[2 * LINE :]
    gather_body(zi[0], lambda: meta[...], low, high, 1, out, whole, None)


def ffn_kernel(layer, sec, rows, ga, ua, da, gb, ub, db, out, wg, wu, wd, gate, up, sems):
    own = sec[0] == layer
    half = wg.shape[0] // 2
    pieces = []
    for a, b, dst, lo, size in (
        (ga, gb, wg, 0, half),
        (ua, ub, wu, 0, half),
        (ga, gb, wg, half, half),
        (ua, ub, wu, half, half),
        (da, db, wd, 0, wd.shape[0]),
    ):
        part = pl.ds(lo, size)
        n = len(pieces)
        pieces.append(
            (
                pltpu.make_async_copy(a.at[part], dst.at[part], sems.at[n]),
                pltpu.make_async_copy(b.at[part], dst.at[part], sems.at[n]),
            )
        )

    @pl.when(own)
    def _():
        for mine, _ in pieces:
            mine.start()

    @pl.when(jnp.logical_not(own))
    def _():
        for _, theirs in pieces:
            theirs.start()

    dot = functools.partial(jnp.dot, preferred_element_type=F32)
    pieces[0][0].wait()
    gate[...] = dot(rows[:, :half], wg[:half])
    pieces[1][0].wait()
    up[...] = dot(rows[:, :half], wu[:half])
    pieces[2][0].wait()
    gate[...] += dot(rows[:, half:], wg[half:])
    pieces[3][0].wait()
    v = gate[...]
    hidden = (v / (1.0 + jnp.exp(-v)) * (up[...] + dot(rows[:, half:], wu[half:]))).astype(BF)
    pieces[4][0].wait()
    out[...] = dot(hidden, wd[...]).astype(BF)


def combine_kernel(layer, zi, meta, rows, *outs):
    tok = 64
    half = rows.shape[1] // 2
    table = meta[:, layer * 32 : layer * 32 + 24].astype(F32)
    holder = table[:, :8].astype(jnp.int32)
    rank = table[:, 8:16].astype(jnp.int32)
    block = lax.broadcasted_iota(jnp.int32, holder.shape, 0) // tok
    place = ((holder // 32) * 4 + holder % 4) * (LINE * CAP) + block * CAP + rank
    slot = jnp.where((holder // 4) % LINE == zi[0], place, -1)
    total = rows.shape[0]
    for i in range(0, LINE, 2):
        part = slice(i * tok, (i + 2) * tok)
        index = lax.broadcasted_iota(jnp.int32, (2 * tok, total), 1)
        mix = jnp.zeros((2 * tok, total), F32)
        for k in range(8):
            mix = jnp.where(index == slot[part, k : k + 1], table[part, 16 + k : 17 + k], mix)
        mix = mix.astype(BF)
        for c in range(2):
            total_rows = jnp.dot(mix, rows[:, c * half : (c + 1) * half], preferred_element_type=F32)
            for b in range(2):
                outs[2 * (i + b) + c][...] = total_rows[b * tok : (b + 1) * tok].astype(BF)


def middle_kernel(sec, start, mine, theirs, *refs):
    f0, f1, b0, b1, p0, p1, kept, low, high = refs
    half = f0.shape[1]
    add = lambda x, y, z: x[...].astype(F32) + y[...].astype(F32) + z[...].astype(F32)
    hidden = start[...].astype(F32) + jnp.concatenate([add(p0, f0, b0), add(p1, f1, b1)], axis=1)
    hidden = hidden.astype(BF)
    kept[...] = hidden
    gain = gain_of(jnp.where(sec[0] == 0, theirs[:16, :], mine[:16, :]))
    normed = normalized(hidden.astype(F32), gain)
    low[...] = normed[:, :half]
    high[...] = normed[:, half:]


STAGGER = 15000


def stagger_kernel(sec, rows, out):
    @pl.when(sec[0] == 1)
    def _():
        pl.delay(STAGGER)


def last_kernel(hidden, f0, f1, b0, b1, p0, p1, out):
    half = f0.shape[1]
    add = lambda x, y, z: x[...].astype(F32) + y[...].astype(F32) + z[...].astype(F32)
    out[:, :half] = (hidden[:, :half].astype(F32) + add(p0, f0, b0)).astype(BF)
    out[:, half:] = (hidden[:, half:].astype(F32) + add(p1, f1, b1)).astype(BF)


ORDER = (0, -1, 1, -2, 2, -3, 3, 4)


def line_gather(low, high):
    held = {0: (low, high)}
    ahead, behind = (low, high), (low, high)
    for step in (1, 2, 3):
        behind = tuple(shift(p, "z", 1, LINE) for p in behind)
        ahead = tuple(shift(p, "z", -1, LINE) for p in ahead)
        held[-step], held[step] = behind, ahead
    held[4] = (shift(behind[0], "z", 1, LINE), shift(ahead[1], "z", -1, LINE))
    return [held[o][0] for o in ORDER], [held[o][1] for o in ORDER]


def line_scatter(parts):
    low = {o: parts[2 * i] for i, o in enumerate(ORDER)}
    high = {o: parts[2 * i + 1] for i, o in enumerate(ORDER)}
    up = lambda p: shift(p, "z", 1, LINE)
    down = lambda p: shift(p, "z", -1, LINE)
    f0, b1 = up(low[4]), down(high[4])
    f0, b1 = up(low[3] + f0), down(high[-3] + b1)
    f1, b0 = up(high[3]), down(low[-3])
    for step in (2, 1):
        f0, f1 = up(low[step] + f0), up(high[step] + f1)
        b0, b1 = down(low[-step] + b0), down(high[-step] + b1)
    return f0, f1, b0, b1, low[0], high[0]


def plane_exchange(rows):
    parts = rows.reshape(16, rows.shape[0] // 16, rows.shape[1])
    return lax.all_to_all(parts, ("x", "y"), 0, 0, tiled=True).reshape(rows.shape)


def local(
    tokens, norm_gain, gate_weight, up_weight, down_weight, expert_place, expert_ids, route_weights
):
    section = lax.axis_index("section").astype(jnp.int32)[None]
    plane = lax.axis_index("z").astype(jnp.int32)[None]
    tok, width = tokens.shape[1], tokens.shape[2]
    half = width // 2
    slots = 16 * LINE * CAP
    lanes = LINE * tok
    ffe = gate_weight.shape[3]
    sds = jax.ShapeDtypeStruct
    anywhere = pl.BlockSpec(memory_space=HBM)

    swap = lambda v: shift(v, "section", 1, 2)
    ids = jnp.swapaxes(expert_ids[0], 1, 2)
    wts = jnp.swapaxes(route_weights[0], 1, 2)
    mine, start = pl.pallas_call(
        pack_kernel,
        out_shape=(sds((56, 128), F32), sds((tok, width), BF)),
        in_specs=[smem()] + [anywhere] * 5,
        out_specs=(vmem(), vmem()),
        scratch_shapes=[
            pltpu.VMEM((1, width), F32),
            pltpu.VMEM((1, 128), jnp.int32),
            pltpu.VMEM((2, 8, tok), jnp.int32),
            pltpu.VMEM((2, 8, tok), F32),
            pltpu.SemaphoreType.DMA((5,)),
        ],
        compiler_params=params(8),
        name="pack",
    )(section, *(pltpu.with_memory_space_constraint(v, HBM) for v in (tokens, norm_gain, expert_place, ids, wts)))
    theirs = swap(mine)

    low, high = pl.pallas_call(
        prepare_kernel,
        out_shape=(sds((tok, half), BF), sds((tok, half + 128), BF)),
        in_specs=[smem()] + [vmem()] * 3,
        out_specs=(vmem(), vmem()),
        compiler_params=params(16),
        name="prepare",
    )(section, start, mine, theirs)

    def experts(rows, layer, mats, mats_b):
        return pl.pallas_call(
            functools.partial(ffn_kernel, layer),
            out_shape=sds((slots, width), BF),
            in_specs=[smem(), vmem()] + [anywhere] * 3 + [pl.BlockSpec(memory_space=pl.ANY)] * 3,
            out_specs=vmem(),
            scratch_shapes=[
                pltpu.VMEM((width, ffe), BF),
                pltpu.VMEM((width, ffe), BF),
                pltpu.VMEM((ffe, width), BF),
                pltpu.VMEM((slots, ffe), F32),
                pltpu.VMEM((slots, ffe), F32),
                pltpu.SemaphoreType.DMA((5,)),
            ],
            compiler_params=params(32),
            name="experts",
        )(section, rows, *mats, *mats_b)

    def combine(rows, meta, layer):
        return pl.pallas_call(
            functools.partial(combine_kernel, layer),
            out_shape=[sds((tok, half), BF)] * (2 * LINE),
            in_specs=[smem(), vmem(), vmem()],
            out_specs=[vmem()] * (2 * LINE),
            compiler_params=params(20),
            name="combine",
        )(plane, meta, rows)

    gather_scratch = [pltpu.VMEM((lanes, width), BF)]
    lows, highs = line_gather(low, high)
    outgoing, meta = pl.pallas_call(
        gather_first_kernel,
        out_shape=(sds((slots, width), BF), sds((lanes, 128), BF)),
        in_specs=[smem()] + [vmem()] * (2 * LINE),
        out_specs=(vmem(), vmem()),
        scratch_shapes=gather_scratch,
        compiler_params=params(20),
        name="spread",
    )(plane, *lows, *highs)

    mats = (gate_weight[0, 0], up_weight[0, 0], down_weight[0, 0])
    outgoing, mats = lax.optimization_barrier((outgoing, mats))
    mats_b = tuple(swap(m) for m in mats)
    mats = tuple(pltpu.with_memory_space_constraint(m, HBM) for m in mats)
    outgoing = pl.pallas_call(
        stagger_kernel,
        out_shape=sds((slots, width), BF),
        in_specs=[smem(), vmem()],
        out_specs=vmem(),
        input_output_aliases={1: 0},
        compiler_params=params(8),
        name="stagger",
    )(section, outgoing)
    arrived = plane_exchange(outgoing)
    returned = plane_exchange(experts(arrived, 0, mats, mats_b))
    sums = line_scatter(combine(returned, meta, 0))

    hidden, low, high = pl.pallas_call(
        middle_kernel,
        out_shape=(sds((tok, width), BF), sds((tok, half), BF), sds((tok, half), BF)),
        in_specs=[smem()] + [vmem()] * 9,
        out_specs=(vmem(), vmem(), vmem()),
        compiler_params=params(16),
        name="middle",
    )(section, start, mine, theirs, *sums)

    lows, highs = line_gather(low, high)
    outgoing = pl.pallas_call(
        gather_later_kernel,
        out_shape=sds((slots, width), BF),
        in_specs=[smem()] + [vmem()] * (2 * LINE + 1),
        out_specs=vmem(),
        scratch_shapes=gather_scratch,
        compiler_params=params(20),
        name="spread_later",
    )(plane, meta, *lows, *highs)
    returned = plane_exchange(experts(plane_exchange(outgoing), 1, mats, mats_b))
    sums = line_scatter(combine(returned, meta, 1))

    final = pl.pallas_call(
        last_kernel,
        out_shape=sds((tok, width), BF),
        in_specs=[vmem()] * 7,
        out_specs=vmem(),
        compiler_params=params(16),
        name="last",
    )(hidden, *sums)
    theirs = swap(final)
    mine_first = section[0] == 0
    return jnp.stack([jnp.where(mine_first, final, theirs), jnp.where(mine_first, theirs, final)])


def solution(mesh):
    fine = Mesh(mesh.devices.reshape(2, 4, 8, 4), ("section", "x", "z", "y"))
    line = ("x", "z", "y")
    in_specs = (
        P(None, line, None),
        P("section", None),
        P("section", line, None, None),
        P("section", line, None, None),
        P("section", line, None, None),
        P("section", None),
        P("section", None, line, None),
        P("section", None, line, None),
    )
    return jax.shard_map(
        local, mesh=fine, in_specs=in_specs, out_specs=P(None, line, None), check_vma=False
    )
```

```python
import functools

import jax
import jax.numpy as jnp
from jax import lax
from jax.experimental import pallas as pl
from jax.experimental.pallas import tpu as pltpu
from jax.sharding import Mesh, PartitionSpec as P

EPSILON = 1e-06
LINE = 8
CAP = 5
BF = jnp.bfloat16
F32 = jnp.float32
VMEM = pltpu.MemorySpace.VMEM
SMEM = pltpu.MemorySpace.SMEM
HBM = pltpu.MemorySpace.HBM


def vmem():
    return pl.BlockSpec(memory_space=VMEM)


def smem():
    return pl.BlockSpec(memory_space=SMEM)


def params(mib):
    return pltpu.CompilerParams(vmem_limit_bytes=mib << 20)


def shift(array, axis, by, size):
    return lax.ppermute(array, axis, [(i, (i + by) % size) for i in range(size)])


def normalized(hidden, gain):
    inverse = lax.rsqrt(jnp.mean(hidden * hidden, axis=-1, keepdims=True) + EPSILON)
    return (hidden * inverse * gain).astype(BF)


def routing_rows(ids, weights, place_row):
    tok = ids.shape[1]
    experts = lax.broadcasted_iota(jnp.int32, (128, tok), 0).astype(F32)
    hits = [(ids[k : k + 1, :] == experts).astype(F32) for k in range(8)]
    has = functools.reduce(jnp.add, hits)
    earlier = (
        lax.broadcasted_iota(jnp.int32, (tok, tok), 0) < lax.broadcasted_iota(jnp.int32, (tok, tok), 1)
    ).astype(F32)
    dot = functools.partial(jnp.dot, preferred_element_type=F32)
    before = dot(has.astype(BF), earlier.astype(BF))
    places = jnp.broadcast_to(place_row, (8, 128)).astype(BF)
    holders = [dot(places, h.astype(BF))[:1] for h in hits]
    positions = [jnp.sum(h * before, axis=0, keepdims=True) for h in hits]
    return jnp.concatenate(holders + positions + [weights, jnp.zeros_like(weights)], axis=0)


def pack_kernel(sec, tok, gain, place, ids, wts, table, hidden, gain_v, place_v, ids_v, wts_v, sems):
    copies = [
        pltpu.make_async_copy(gain, gain_v, sems.at[0]),
        pltpu.make_async_copy(place, place_v, sems.at[1]),
        pltpu.make_async_copy(ids, ids_v, sems.at[2]),
        pltpu.make_async_copy(wts, wts_v, sems.at[3]),
        pltpu.make_async_copy(tok.at[sec[0]], hidden, sems.at[4]),
    ]
    for c in copies:
        c.start()
    table[...] = jnp.zeros(table.shape, F32)
    for c in copies[:4]:
        c.wait()
    for i in range(16):
        table[i : i + 1, :] = gain_v[:, 128 * i : 128 * (i + 1)]
    for m in range(2):
        table[16 + 8 * m : 24 + 8 * m, :64] = ids_v[m].astype(F32)
        table[32 + 8 * m : 40 + 8 * m, :64] = wts_v[m]
    table[48:49, :] = place_v[...].astype(F32)
    copies[4].wait()


def gain_of(table):
    return jnp.concatenate([table[i : i + 1, :] for i in range(16)], axis=1)


def prepare_kernel(sec, hidden, mine, theirs, low, high):
    s = sec[0]
    first = jnp.where(s == 0, mine[...], theirs[...])
    second = jnp.where(s == 0, theirs[...], mine[...])
    half = hidden.shape[1] // 2
    normed = normalized(hidden[...].astype(F32), gain_of(first))
    low[...] = normed[:, :half]
    high[:, :half] = normed[:, half:]
    rows = []
    for table in (first, second):
        ids = jnp.where(s == 0, table[16:24, :64], table[24:32, :64])
        wts = jnp.where(s == 0, table[32:40, :64], table[40:48, :64])
        rows.append(routing_rows(ids, wts, table[48:49, :]))
    table = jnp.concatenate(rows, axis=0)
    table = jnp.concatenate([table, jnp.zeros_like(table)], axis=1)
    table = jnp.concatenate([table, jnp.zeros_like(table)], axis=0)
    high[:, half:] = table.T[: hidden.shape[0], :].astype(BF)


def gather_body(zi, metas, blocks_low, blocks_high, layer, out, whole, emit):
    tok = 64
    half = whole.shape[1] // 2
    for i in range(LINE):
        whole[i * tok : (i + 1) * tok, :half] = blocks_low[i][...]
        whole[i * tok : (i + 1) * tok, half:] = blocks_high[i][:, :half]
    meta = metas()
    if emit is not None:
        emit[...] = meta
    rows = meta.astype(F32).T[layer * 32 : layer * 32 + 16, :]
    holder = rows[:8].astype(jnp.int32)
    rank = rows[8:].astype(jnp.int32)
    block = lax.broadcasted_iota(jnp.int32, holder.shape, 1) // tok
    place = ((holder // 32) * 4 + holder % 4) * (LINE * CAP) + block * CAP + rank
    slot = jnp.where((holder // 4) % LINE == zi, place, -1)
    total = out.shape[0]
    lanes = LINE * tok
    step = 128
    for r in range(0, total, step):
        index = lax.broadcasted_iota(jnp.int32, (step, lanes), 0) + r
        hit = index == slot[0:1, :]
        for k in range(1, 8):
            hit = jnp.logical_or(hit, index == slot[k : k + 1, :])
        pick = jnp.where(hit, 1.0, 0.0).astype(BF)
        out[r : r + step, :] = jnp.dot(pick, whole[...], preferred_element_type=F32).astype(BF)


def gather_first_kernel(zi, *refs):
    low, high = refs[:LINE], refs[LINE : 2 * LINE]
    out, emit, whole = refs[2 * LINE :]
    half = low[0].shape[1]
    metas = lambda: jnp.concatenate([h[:, half:] for h in high], axis=0)
    gather_body(zi[0], metas, low, high, 0, out, whole, emit)


def gather_later_kernel(zi, meta, *refs):
    low, high = refs[:LINE], refs[LINE : 2 * LINE]
    out, whole = refs[2 * LINE :]
    gather_body(zi[0], lambda: meta[...], low, high, 1, out, whole, None)


def ffn_kernel(layer, sec, rows, ga, ua, da, gb, ub, db, out, wg, wu, wd, gate, up, sems):
    own = sec[0] == layer
    half = wg.shape[0] // 2
    pieces = []
    for a, b, dst, lo, size in (
        (ga, gb, wg, 0, half),
        (ua, ub, wu, 0, half),
        (ga, gb, wg, half, half),
        (ua, ub, wu, half, half),
        (da, db, wd, 0, wd.shape[0]),
    ):
        part = pl.ds(lo, size)
        n = len(pieces)
        pieces.append(
            (
                pltpu.make_async_copy(a.at[part], dst.at[part], sems.at[n]),
                pltpu.make_async_copy(b.at[part], dst.at[part], sems.at[n]),
            )
        )

    @pl.when(own)
    def _():
        for mine, _ in pieces:
            mine.start()

    @pl.when(jnp.logical_not(own))
    def _():
        for _, theirs in pieces:
            theirs.start()

    dot = functools.partial(jnp.dot, preferred_element_type=F32)
    pieces[0][0].wait()
    gate[...] = dot(rows[:, :half], wg[:half])
    pieces[1][0].wait()
    up[...] = dot(rows[:, :half], wu[:half])
    pieces[2][0].wait()
    gate[...] += dot(rows[:, half:], wg[half:])
    pieces[3][0].wait()
    v = gate[...]
    hidden = (v / (1.0 + jnp.exp(-v)) * (up[...] + dot(rows[:, half:], wu[half:]))).astype(BF)
    pieces[4][0].wait()
    out[...] = dot(hidden, wd[...]).astype(BF)


def combine_kernel(layer, zi, meta, rows, *outs):
    tok = 64
    half = rows.shape[1] // 2
    table = meta[:, layer * 32 : layer * 32 + 24].astype(F32)
    holder = table[:, :8].astype(jnp.int32)
    rank = table[:, 8:16].astype(jnp.int32)
    block = lax.broadcasted_iota(jnp.int32, holder.shape, 0) // tok
    place = ((holder // 32) * 4 + holder % 4) * (LINE * CAP) + block * CAP + rank
    slot = jnp.where((holder // 4) % LINE == zi[0], place, -1)
    total = rows.shape[0]
    for i in range(0, LINE, 2):
        part = slice(i * tok, (i + 2) * tok)
        index = lax.broadcasted_iota(jnp.int32, (2 * tok, total), 1)
        mix = jnp.zeros((2 * tok, total), F32)
        for k in range(8):
            mix = jnp.where(index == slot[part, k : k + 1], table[part, 16 + k : 17 + k], mix)
        mix = mix.astype(BF)
        for c in range(2):
            total_rows = jnp.dot(mix, rows[:, c * half : (c + 1) * half], preferred_element_type=F32)
            for b in range(2):
                outs[2 * (i + b) + c][...] = total_rows[b * tok : (b + 1) * tok].astype(BF)


def middle_kernel(sec, start, mine, theirs, *refs):
    f0, f1, b0, b1, p0, p1, kept, low, high = refs
    half = f0.shape[1]
    add = lambda x, y, z: x[...].astype(F32) + y[...].astype(F32) + z[...].astype(F32)
    hidden = start[...].astype(F32) + jnp.concatenate([add(p0, f0, b0), add(p1, f1, b1)], axis=1)
    hidden = hidden.astype(BF)
    kept[...] = hidden
    gain = gain_of(jnp.where(sec[0] == 0, theirs[:16, :], mine[:16, :]))
    normed = normalized(hidden.astype(F32), gain)
    low[...] = normed[:, :half]
    high[...] = normed[:, half:]


STAGGER = (12000, 8000)


def stagger_kernel(wait, sec, rows, out):
    @pl.when(sec[0] == 1)
    def _():
        pl.delay(wait)


def last_kernel(hidden, f0, f1, b0, b1, p0, p1, out):
    half = f0.shape[1]
    add = lambda x, y, z: x[...].astype(F32) + y[...].astype(F32) + z[...].astype(F32)
    out[:, :half] = (hidden[:, :half].astype(F32) + add(p0, f0, b0)).astype(BF)
    out[:, half:] = (hidden[:, half:].astype(F32) + add(p1, f1, b1)).astype(BF)


ORDER = (0, -1, 1, -2, 2, -3, 3, 4)


def line_gather(low, high):
    held = {0: (low, high)}
    ahead, behind = (low, high), (low, high)
    for step in (1, 2, 3):
        behind = tuple(shift(p, "z", 1, LINE) for p in behind)
        ahead = tuple(shift(p, "z", -1, LINE) for p in ahead)
        held[-step], held[step] = behind, ahead
    held[4] = (shift(behind[0], "z", 1, LINE), shift(ahead[1], "z", -1, LINE))
    return [held[o][0] for o in ORDER], [held[o][1] for o in ORDER]


def line_scatter(parts):
    low = {o: parts[2 * i] for i, o in enumerate(ORDER)}
    high = {o: parts[2 * i + 1] for i, o in enumerate(ORDER)}
    up = lambda p: shift(p, "z", 1, LINE)
    down = lambda p: shift(p, "z", -1, LINE)
    f0, b1 = up(low[4]), down(high[4])
    f0, b1 = up(low[3] + f0), down(high[-3] + b1)
    f1, b0 = up(high[3]), down(low[-3])
    for step in (2, 1):
        f0, f1 = up(low[step] + f0), up(high[step] + f1)
        b0, b1 = down(low[-step] + b0), down(high[-step] + b1)
    return f0, f1, b0, b1, low[0], high[0]


def plane_exchange(rows):
    parts = rows.reshape(16, rows.shape[0] // 16, rows.shape[1])
    return lax.all_to_all(parts, ("x", "y"), 0, 0, tiled=True).reshape(rows.shape)


def local(
    tokens, norm_gain, gate_weight, up_weight, down_weight, expert_place, expert_ids, route_weights
):
    section = lax.axis_index("section").astype(jnp.int32)[None]
    plane = lax.axis_index("z").astype(jnp.int32)[None]
    tok, width = tokens.shape[1], tokens.shape[2]
    half = width // 2
    slots = 16 * LINE * CAP
    lanes = LINE * tok
    ffe = gate_weight.shape[3]
    sds = jax.ShapeDtypeStruct
    anywhere = pl.BlockSpec(memory_space=HBM)

    swap = lambda v: shift(v, "section", 1, 2)
    ids = jnp.swapaxes(expert_ids[0], 1, 2)
    wts = jnp.swapaxes(route_weights[0], 1, 2)
    mine, start = pl.pallas_call(
        pack_kernel,
        out_shape=(sds((56, 128), F32), sds((tok, width), BF)),
        in_specs=[smem()] + [anywhere] * 5,
        out_specs=(vmem(), vmem()),
        scratch_shapes=[
            pltpu.VMEM((1, width), F32),
            pltpu.VMEM((1, 128), jnp.int32),
            pltpu.VMEM((2, 8, tok), jnp.int32),
            pltpu.VMEM((2, 8, tok), F32),
            pltpu.SemaphoreType.DMA((5,)),
        ],
        compiler_params=params(8),
        name="pack",
    )(section, *(pltpu.with_memory_space_constraint(v, HBM) for v in (tokens, norm_gain, expert_place, ids, wts)))
    theirs = swap(mine)

    low, high = pl.pallas_call(
        prepare_kernel,
        out_shape=(sds((tok, half), BF), sds((tok, half + 128), BF)),
        in_specs=[smem()] + [vmem()] * 3,
        out_specs=(vmem(), vmem()),
        compiler_params=params(16),
        name="prepare",
    )(section, start, mine, theirs)

    def experts(rows, layer, mats, mats_b):
        return pl.pallas_call(
            functools.partial(ffn_kernel, layer),
            out_shape=sds((slots, width), BF),
            in_specs=[smem(), vmem()] + [anywhere] * 3 + [pl.BlockSpec(memory_space=pl.ANY)] * 3,
            out_specs=vmem(),
            scratch_shapes=[
                pltpu.VMEM((width, ffe), BF),
                pltpu.VMEM((width, ffe), BF),
                pltpu.VMEM((ffe, width), BF),
                pltpu.VMEM((slots, ffe), F32),
                pltpu.VMEM((slots, ffe), F32),
                pltpu.SemaphoreType.DMA((5,)),
            ],
            compiler_params=params(32),
            name="experts",
        )(section, rows, *mats, *mats_b)

    def combine(rows, meta, layer):
        return pl.pallas_call(
            functools.partial(combine_kernel, layer),
            out_shape=[sds((tok, half), BF)] * (2 * LINE),
            in_specs=[smem(), vmem(), vmem()],
            out_specs=[vmem()] * (2 * LINE),
            compiler_params=params(20),
            name="combine",
        )(plane, meta, rows)

    def stagger(rows, layer):
        return pl.pallas_call(
            functools.partial(stagger_kernel, STAGGER[layer]),
            out_shape=sds((slots, width), BF),
            in_specs=[smem(), vmem()],
            out_specs=vmem(),
            input_output_aliases={1: 0},
            compiler_params=params(8),
            name="stagger",
        )(section, rows)

    gather_scratch = [pltpu.VMEM((lanes, width), BF)]
    lows, highs = line_gather(low, high)
    outgoing, meta = pl.pallas_call(
        gather_first_kernel,
        out_shape=(sds((slots, width), BF), sds((lanes, 128), BF)),
        in_specs=[smem()] + [vmem()] * (2 * LINE),
        out_specs=(vmem(), vmem()),
        scratch_shapes=gather_scratch,
        compiler_params=params(20),
        name="spread",
    )(plane, *lows, *highs)

    mats = (gate_weight[0, 0], up_weight[0, 0], down_weight[0, 0])
    outgoing, mats = lax.optimization_barrier((outgoing, mats))
    mats_b = tuple(swap(m) for m in mats)
    mats = tuple(pltpu.with_memory_space_constraint(m, HBM) for m in mats)
    arrived = plane_exchange(stagger(outgoing, 0))
    returned = plane_exchange(experts(arrived, 0, mats, mats_b))
    sums = line_scatter(combine(returned, meta, 0))

    hidden, low, high = pl.pallas_call(
        middle_kernel,
        out_shape=(sds((tok, width), BF), sds((tok, half), BF), sds((tok, half), BF)),
        in_specs=[smem()] + [vmem()] * 9,
        out_specs=(vmem(), vmem(), vmem()),
        compiler_params=params(16),
        name="middle",
    )(section, start, mine, theirs, *sums)

    lows, highs = line_gather(low, high)
    outgoing = pl.pallas_call(
        gather_later_kernel,
        out_shape=sds((slots, width), BF),
        in_specs=[smem()] + [vmem()] * (2 * LINE + 1),
        out_specs=vmem(),
        scratch_shapes=gather_scratch,
        compiler_params=params(20),
        name="spread_later",
    )(plane, meta, *lows, *highs)
    returned = plane_exchange(experts(plane_exchange(stagger(outgoing, 1)), 1, mats, mats_b))
    sums = line_scatter(combine(returned, meta, 1))

    final = pl.pallas_call(
        last_kernel,
        out_shape=sds((tok, width), BF),
        in_specs=[vmem()] * 7,
        out_specs=vmem(),
        compiler_params=params(16),
        name="last",
    )(hidden, *sums)
    theirs = swap(final)
    mine_first = section[0] == 0
    return jnp.stack([jnp.where(mine_first, final, theirs), jnp.where(mine_first, theirs, final)])


def solution(mesh):
    fine = Mesh(mesh.devices.reshape(2, 4, 8, 4), ("section", "x", "z", "y"))
    line = ("x", "z", "y")
    in_specs = (
        P(None, line, None),
        P("section", None),
        P("section", line, None, None),
        P("section", line, None, None),
        P("section", line, None, None),
        P("section", None),
        P("section", None, line, None),
        P("section", None, line, None),
    )
    return jax.shard_map(
        local, mesh=fine, in_specs=in_specs, out_specs=P(None, line, None), check_vma=False
    )
```

```python
import functools

import jax
import jax.numpy as jnp
from jax import lax
from jax.experimental import pallas as pl
from jax.experimental.pallas import tpu as pltpu
from jax.sharding import Mesh, PartitionSpec as P

EPSILON = 1e-06
LINE = 8
CAP = 5
BF = jnp.bfloat16
F32 = jnp.float32
VMEM = pltpu.MemorySpace.VMEM
SMEM = pltpu.MemorySpace.SMEM
HBM = pltpu.MemorySpace.HBM


def vmem():
    return pl.BlockSpec(memory_space=VMEM)


def smem():
    return pl.BlockSpec(memory_space=SMEM)


def params(mib):
    return pltpu.CompilerParams(vmem_limit_bytes=mib << 20)


def shift(array, axis, by, size):
    return lax.ppermute(array, axis, [(i, (i + by) % size) for i in range(size)])


def normalized(hidden, gain):
    inverse = lax.rsqrt(jnp.mean(hidden * hidden, axis=-1, keepdims=True) + EPSILON)
    return (hidden * inverse * gain).astype(BF)


def routing_rows(ids, weights, place_row):
    tok = ids.shape[1]
    experts = lax.broadcasted_iota(jnp.int32, (128, tok), 0).astype(F32)
    hits = [(ids[k : k + 1, :] == experts).astype(F32) for k in range(8)]
    has = functools.reduce(jnp.add, hits)
    earlier = (
        lax.broadcasted_iota(jnp.int32, (tok, tok), 0) < lax.broadcasted_iota(jnp.int32, (tok, tok), 1)
    ).astype(F32)
    dot = functools.partial(jnp.dot, preferred_element_type=F32)
    before = dot(has.astype(BF), earlier.astype(BF))
    places = jnp.broadcast_to(place_row, (8, 128)).astype(BF)
    holders = [dot(places, h.astype(BF))[:1] for h in hits]
    positions = [jnp.sum(h * before, axis=0, keepdims=True) for h in hits]
    return jnp.concatenate(holders + positions + [weights, jnp.zeros_like(weights)], axis=0)


def pack_kernel(sec, tok, gain, place, ids, wts, table, hidden, gain_v, place_v, ids_v, wts_v, sems):
    copies = [
        pltpu.make_async_copy(gain, gain_v, sems.at[0]),
        pltpu.make_async_copy(place, place_v, sems.at[1]),
        pltpu.make_async_copy(ids, ids_v, sems.at[2]),
        pltpu.make_async_copy(wts, wts_v, sems.at[3]),
        pltpu.make_async_copy(tok.at[sec[0]], hidden, sems.at[4]),
    ]
    for c in copies:
        c.start()
    table[...] = jnp.zeros(table.shape, F32)
    for c in copies[:4]:
        c.wait()
    for i in range(16):
        table[i : i + 1, :] = gain_v[:, 128 * i : 128 * (i + 1)]
    for m in range(2):
        table[16 + 8 * m : 24 + 8 * m, :64] = ids_v[m].astype(F32)
        table[32 + 8 * m : 40 + 8 * m, :64] = wts_v[m]
    table[48:49, :] = place_v[...].astype(F32)
    copies[4].wait()


def gain_of(table):
    return jnp.concatenate([table[i : i + 1, :] for i in range(16)], axis=1)


def prepare_kernel(sec, hidden, mine, theirs, low, high):
    s = sec[0]
    first = jnp.where(s == 0, mine[...], theirs[...])
    second = jnp.where(s == 0, theirs[...], mine[...])
    half = hidden.shape[1] // 2
    normed = normalized(hidden[...].astype(F32), gain_of(first))
    low[...] = normed[:, :half]
    high[:, :half] = normed[:, half:]
    rows = []
    for table in (first, second):
        ids = jnp.where(s == 0, table[16:24, :64], table[24:32, :64])
        wts = jnp.where(s == 0, table[32:40, :64], table[40:48, :64])
        rows.append(routing_rows(ids, wts, table[48:49, :]))
    table = jnp.concatenate(rows, axis=0)
    table = jnp.concatenate([table, jnp.zeros_like(table)], axis=1)
    table = jnp.concatenate([table, jnp.zeros_like(table)], axis=0)
    high[:, half:] = table.T[: hidden.shape[0], :].astype(BF)


def gather_body(zi, metas, blocks_low, blocks_high, layer, out, whole, emit):
    tok = 64
    half = whole.shape[1] // 2
    for i in range(LINE):
        whole[i * tok : (i + 1) * tok, :half] = blocks_low[i][...]
        whole[i * tok : (i + 1) * tok, half:] = blocks_high[i][:, :half]
    meta = metas()
    if emit is not None:
        emit[...] = meta
    rows = meta.astype(F32).T[layer * 32 : layer * 32 + 16, :]
    holder = rows[:8].astype(jnp.int32)
    rank = rows[8:].astype(jnp.int32)
    block = lax.broadcasted_iota(jnp.int32, holder.shape, 1) // tok
    place = ((holder // 32) * 4 + holder % 4) * (LINE * CAP) + block * CAP + rank
    slot = jnp.where((holder // 4) % LINE == zi, place, -1)
    total = out.shape[0]
    lanes = LINE * tok
    step = 128
    for r in range(0, total, step):
        index = lax.broadcasted_iota(jnp.int32, (step, lanes), 0) + r
        hit = index == slot[0:1, :]
        for k in range(1, 8):
            hit = jnp.logical_or(hit, index == slot[k : k + 1, :])
        pick = jnp.where(hit, 1.0, 0.0).astype(BF)
        out[r : r + step, :] = jnp.dot(pick, whole[...], preferred_element_type=F32).astype(BF)


def gather_first_kernel(zi, *refs):
    low, high = refs[:LINE], refs[LINE : 2 * LINE]
    out, emit, whole = refs[2 * LINE :]
    half = low[0].shape[1]
    metas = lambda: jnp.concatenate([h[:, half:] for h in high], axis=0)
    gather_body(zi[0], metas, low, high, 0, out, whole, emit)


def gather_later_kernel(zi, meta, *refs):
    low, high = refs[:LINE], refs[LINE : 2 * LINE]
    out, whole = refs[2 * LINE :]
    gather_body(zi[0], lambda: meta[...], low, high, 1, out, whole, None)


def ffn_kernel(layer, sec, rows, ga, ua, da, gb, ub, db, out, wg, wu, wd, gate, up, sems):
    own = sec[0] == layer
    half = wg.shape[0] // 2
    pieces = []
    for a, b, dst, lo, size in (
        (ga, gb, wg, 0, half),
        (ua, ub, wu, 0, half),
        (ga, gb, wg, half, half),
        (ua, ub, wu, half, half),
        (da, db, wd, 0, wd.shape[0]),
    ):
        part = pl.ds(lo, size)
        n = len(pieces)
        pieces.append(
            (
                pltpu.make_async_copy(a.at[part], dst.at[part], sems.at[n]),
                pltpu.make_async_copy(b.at[part], dst.at[part], sems.at[n]),
            )
        )

    @pl.when(own)
    def _():
        for mine, _ in pieces:
            mine.start()

    @pl.when(jnp.logical_not(own))
    def _():
        for _, theirs in pieces:
            theirs.start()

    dot = functools.partial(jnp.dot, preferred_element_type=F32)
    pieces[0][0].wait()
    gate[...] = dot(rows[:, :half], wg[:half])
    pieces[1][0].wait()
    up[...] = dot(rows[:, :half], wu[:half])
    pieces[2][0].wait()
    gate[...] += dot(rows[:, half:], wg[half:])
    pieces[3][0].wait()
    v = gate[...]
    hidden = (v / (1.0 + jnp.exp(-v)) * (up[...] + dot(rows[:, half:], wu[half:]))).astype(BF)
    pieces[4][0].wait()
    out[...] = dot(hidden, wd[...]).astype(BF)


def combine_kernel(layer, first, zi, meta, rows, *outs):
    tok = 64
    half = rows.shape[1] // 2
    total = rows.shape[0]
    count = len(outs) // 2
    table = meta[first * tok : (first + count) * tok, layer * 32 : layer * 32 + 24].astype(F32)
    holder = table[:, :8].astype(jnp.int32)
    rank = table[:, 8:16].astype(jnp.int32)
    block = lax.broadcasted_iota(jnp.int32, holder.shape, 0) // tok + first
    place = ((holder // 32) * 4 + holder % 4) * (LINE * CAP) + block * CAP + rank
    slot = jnp.where((holder // 4) % LINE == zi[0], place, -1)
    for i in range(0, count, 2):
        size = min(2, count - i)
        part = slice(i * tok, (i + size) * tok)
        index = lax.broadcasted_iota(jnp.int32, (size * tok, total), 1)
        mix = jnp.zeros((size * tok, total), F32)
        for k in range(8):
            mix = jnp.where(index == slot[part, k : k + 1], table[part, 16 + k : 17 + k], mix)
        mix = mix.astype(BF)
        for c in range(2):
            sums = jnp.dot(mix, rows[:, c * half : (c + 1) * half], preferred_element_type=F32)
            for b in range(size):
                outs[2 * (i + b) + c][...] = sums[b * tok : (b + 1) * tok].astype(BF)


def middle_kernel(sec, start, mine, theirs, *refs):
    f0, f1, b0, b1, p0, p1, kept, low, high = refs
    half = f0.shape[1]
    add = lambda x, y, z: x[...].astype(F32) + y[...].astype(F32) + z[...].astype(F32)
    hidden = start[...].astype(F32) + jnp.concatenate([add(p0, f0, b0), add(p1, f1, b1)], axis=1)
    hidden = hidden.astype(BF)
    kept[...] = hidden
    gain = gain_of(jnp.where(sec[0] == 0, theirs[:16, :], mine[:16, :]))
    normed = normalized(hidden.astype(F32), gain)
    low[...] = normed[:, :half]
    high[...] = normed[:, half:]


STAGGER = 14000


def stagger_kernel(sec, rows, out):
    @pl.when(sec[0] == 0)
    def _():
        pl.delay(STAGGER)


def last_kernel(hidden, f0, f1, b0, b1, p0, p1, out):
    half = f0.shape[1]
    add = lambda x, y, z: x[...].astype(F32) + y[...].astype(F32) + z[...].astype(F32)
    out[:, :half] = (hidden[:, :half].astype(F32) + add(p0, f0, b0)).astype(BF)
    out[:, half:] = (hidden[:, half:].astype(F32) + add(p1, f1, b1)).astype(BF)


ORDER = (0, -1, 1, -2, 2, -3, 3, 4)


def line_gather(low, high):
    held = {0: (low, high)}
    ahead, behind = (low, high), (low, high)
    for step in (1, 2, 3):
        behind = tuple(shift(p, "z", 1, LINE) for p in behind)
        ahead = tuple(shift(p, "z", -1, LINE) for p in ahead)
        held[-step], held[step] = behind, ahead
    held[4] = (shift(behind[0], "z", 1, LINE), shift(ahead[1], "z", -1, LINE))
    return [held[o][0] for o in ORDER], [held[o][1] for o in ORDER]


def line_scatter(parts):
    low = {o: parts[2 * i] for i, o in enumerate(ORDER)}
    high = {o: parts[2 * i + 1] for i, o in enumerate(ORDER)}
    up = lambda p: shift(p, "z", 1, LINE)
    down = lambda p: shift(p, "z", -1, LINE)
    f0, b1 = up(low[4]), down(high[4])
    f0, b1 = up(low[3] + f0), down(high[-3] + b1)
    f1, b0 = up(high[3]), down(low[-3])
    for step in (2, 1):
        f0, f1 = up(low[step] + f0), up(high[step] + f1)
        b0, b1 = down(low[-step] + b0), down(high[-step] + b1)
    return f0, f1, b0, b1, low[0], high[0]


def plane_exchange(rows):
    parts = rows.reshape(16, rows.shape[0] // 16, rows.shape[1])
    return lax.all_to_all(parts, ("x", "y"), 0, 0, tiled=True).reshape(rows.shape)


def local(
    tokens, norm_gain, gate_weight, up_weight, down_weight, expert_place, expert_ids, route_weights
):
    section = lax.axis_index("section").astype(jnp.int32)[None]
    plane = lax.axis_index("z").astype(jnp.int32)[None]
    tok, width = tokens.shape[1], tokens.shape[2]
    half = width // 2
    slots = 16 * LINE * CAP
    lanes = LINE * tok
    ffe = gate_weight.shape[3]
    sds = jax.ShapeDtypeStruct
    anywhere = pl.BlockSpec(memory_space=HBM)

    swap = lambda v: shift(v, "section", 1, 2)
    ids = jnp.swapaxes(expert_ids[0], 1, 2)
    wts = jnp.swapaxes(route_weights[0], 1, 2)
    mine, start = pl.pallas_call(
        pack_kernel,
        out_shape=(sds((56, 128), F32), sds((tok, width), BF)),
        in_specs=[smem()] + [anywhere] * 5,
        out_specs=(vmem(), vmem()),
        scratch_shapes=[
            pltpu.VMEM((1, width), F32),
            pltpu.VMEM((1, 128), jnp.int32),
            pltpu.VMEM((2, 8, tok), jnp.int32),
            pltpu.VMEM((2, 8, tok), F32),
            pltpu.SemaphoreType.DMA((5,)),
        ],
        compiler_params=params(8),
        name="pack",
    )(section, *(pltpu.with_memory_space_constraint(v, HBM) for v in (tokens, norm_gain, expert_place, ids, wts)))
    theirs = swap(mine)

    low, high = pl.pallas_call(
        prepare_kernel,
        out_shape=(sds((tok, half), BF), sds((tok, half + 128), BF)),
        in_specs=[smem()] + [vmem()] * 3,
        out_specs=(vmem(), vmem()),
        compiler_params=params(16),
        name="prepare",
    )(section, start, mine, theirs)

    def experts(rows, layer, mats, mats_b):
        return pl.pallas_call(
            functools.partial(ffn_kernel, layer),
            out_shape=sds((slots, width), BF),
            in_specs=[smem(), vmem()] + [anywhere] * 3 + [pl.BlockSpec(memory_space=pl.ANY)] * 3,
            out_specs=vmem(),
            scratch_shapes=[
                pltpu.VMEM((width, ffe), BF),
                pltpu.VMEM((width, ffe), BF),
                pltpu.VMEM((ffe, width), BF),
                pltpu.VMEM((slots, ffe), F32),
                pltpu.VMEM((slots, ffe), F32),
                pltpu.SemaphoreType.DMA((5,)),
            ],
            compiler_params=params(32),
            name="experts",
        )(section, rows, *mats, *mats_b)

    def combine(rows, meta, layer):
        def blocks(first, count):
            return pl.pallas_call(
                functools.partial(combine_kernel, layer, first),
                out_shape=[sds((tok, half), BF)] * (2 * count),
                in_specs=[smem(), vmem(), vmem()],
                out_specs=[vmem()] * (2 * count),
                compiler_params=params(16),
                name="combine",
            )(plane, meta, rows)

        far = blocks(5, 3)
        return list(blocks(0, 5)) + list(far)

    def stagger(rows):
        return pl.pallas_call(
            stagger_kernel,
            out_shape=sds((slots, width), BF),
            in_specs=[smem(), vmem()],
            out_specs=vmem(),
            input_output_aliases={1: 0},
            compiler_params=params(8),
            name="stagger",
        )(section, rows)

    gather_scratch = [pltpu.VMEM((lanes, width), BF)]
    lows, highs = line_gather(low, high)
    outgoing, meta = pl.pallas_call(
        gather_first_kernel,
        out_shape=(sds((slots, width), BF), sds((lanes, 128), BF)),
        in_specs=[smem()] + [vmem()] * (2 * LINE),
        out_specs=(vmem(), vmem()),
        scratch_shapes=gather_scratch,
        compiler_params=params(20),
        name="spread",
    )(plane, *lows, *highs)

    mats = (gate_weight[0, 0], up_weight[0, 0], down_weight[0, 0])
    outgoing, mats = lax.optimization_barrier((outgoing, mats))
    mats_b = tuple(swap(m) for m in mats)
    mats = tuple(pltpu.with_memory_space_constraint(m, HBM) for m in mats)
    arrived = plane_exchange(stagger(outgoing))
    returned = plane_exchange(experts(arrived, 0, mats, mats_b))
    sums = line_scatter(combine(returned, meta, 0))

    hidden, low, high = pl.pallas_call(
        middle_kernel,
        out_shape=(sds((tok, width), BF), sds((tok, half), BF), sds((tok, half), BF)),
        in_specs=[smem()] + [vmem()] * 9,
        out_specs=(vmem(), vmem(), vmem()),
        compiler_params=params(16),
        name="middle",
    )(section, start, mine, theirs, *sums)

    lows, highs = line_gather(low, high)
    outgoing = pl.pallas_call(
        gather_later_kernel,
        out_shape=sds((slots, width), BF),
        in_specs=[smem()] + [vmem()] * (2 * LINE + 1),
        out_specs=vmem(),
        scratch_shapes=gather_scratch,
        compiler_params=params(20),
        name="spread_later",
    )(plane, meta, *lows, *highs)
    returned = plane_exchange(experts(plane_exchange(outgoing), 1, mats, mats_b))
    sums = line_scatter(combine(returned, meta, 1))

    final = pl.pallas_call(
        last_kernel,
        out_shape=sds((tok, width), BF),
        in_specs=[vmem()] * 7,
        out_specs=vmem(),
        compiler_params=params(16),
        name="last",
    )(hidden, *sums)
    theirs = swap(final)
    mine_first = section[0] == 0
    return jnp.stack([jnp.where(mine_first, final, theirs), jnp.where(mine_first, theirs, final)])


def solution(mesh):
    fine = Mesh(mesh.devices.reshape(2, 4, 8, 4), ("section", "x", "z", "y"))
    line = ("x", "z", "y")
    in_specs = (
        P(None, line, None),
        P("section", None),
        P("section", line, None, None),
        P("section", line, None, None),
        P("section", line, None, None),
        P("section", None),
        P("section", None, line, None),
        P("section", None, line, None),
    )
    return jax.shard_map(
        local, mesh=fine, in_specs=in_specs, out_specs=P(None, line, None), check_vma=False
    )
```

```python
import functools

import jax
import jax.numpy as jnp
from jax import lax
from jax.experimental import pallas as pl
from jax.experimental.pallas import tpu as pltpu
from jax.sharding import Mesh, PartitionSpec as P

EPSILON = 1e-06
LINE = 8
CAP = 5
BF = jnp.bfloat16
F32 = jnp.float32
VMEM = pltpu.MemorySpace.VMEM
SMEM = pltpu.MemorySpace.SMEM
HBM = pltpu.MemorySpace.HBM


def vmem():
    return pl.BlockSpec(memory_space=VMEM)


def smem():
    return pl.BlockSpec(memory_space=SMEM)


def params(mib):
    return pltpu.CompilerParams(vmem_limit_bytes=mib << 20)


def shift(array, axis, by, size):
    return lax.ppermute(array, axis, [(i, (i + by) % size) for i in range(size)])


def normalized(hidden, gain):
    inverse = lax.rsqrt(jnp.mean(hidden * hidden, axis=-1, keepdims=True) + EPSILON)
    return (hidden * inverse * gain).astype(BF)


def routing_rows(ids, weights, place_row):
    tok = ids.shape[1]
    experts = lax.broadcasted_iota(jnp.int32, (128, tok), 0).astype(F32)
    hits = [(ids[k : k + 1, :] == experts).astype(F32) for k in range(8)]
    has = functools.reduce(jnp.add, hits)
    earlier = (
        lax.broadcasted_iota(jnp.int32, (tok, tok), 0) < lax.broadcasted_iota(jnp.int32, (tok, tok), 1)
    ).astype(F32)
    dot = functools.partial(jnp.dot, preferred_element_type=F32)
    before = dot(has.astype(BF), earlier.astype(BF))
    places = jnp.broadcast_to(place_row, (8, 128)).astype(BF)
    holders = [dot(places, h.astype(BF))[:1] for h in hits]
    positions = [jnp.sum(h * before, axis=0, keepdims=True) for h in hits]
    return jnp.concatenate(holders + positions + [weights, jnp.zeros_like(weights)], axis=0)


def pack_kernel(sec, tok, gain, place, ids, wts, table, hidden, gain_v, place_v, ids_v, wts_v, sems):
    copies = [
        pltpu.make_async_copy(gain, gain_v, sems.at[0]),
        pltpu.make_async_copy(place, place_v, sems.at[1]),
        pltpu.make_async_copy(ids, ids_v, sems.at[2]),
        pltpu.make_async_copy(wts, wts_v, sems.at[3]),
        pltpu.make_async_copy(tok.at[sec[0]], hidden, sems.at[4]),
    ]
    for c in copies:
        c.start()
    table[...] = jnp.zeros(table.shape, F32)
    for c in copies[:4]:
        c.wait()
    for i in range(16):
        table[i : i + 1, :] = gain_v[:, 128 * i : 128 * (i + 1)]
    for m in range(2):
        table[16 + 8 * m : 24 + 8 * m, :64] = ids_v[m].astype(F32)
        table[32 + 8 * m : 40 + 8 * m, :64] = wts_v[m]
    table[48:49, :] = place_v[...].astype(F32)
    copies[4].wait()


def gain_of(table):
    return jnp.concatenate([table[i : i + 1, :] for i in range(16)], axis=1)


def prepare_kernel(sec, hidden, mine, theirs, low, high):
    s = sec[0]
    first = jnp.where(s == 0, mine[...], theirs[...])
    second = jnp.where(s == 0, theirs[...], mine[...])
    half = hidden.shape[1] // 2
    normed = normalized(hidden[...].astype(F32), gain_of(first))
    low[...] = normed[:, :half]
    high[:, :half] = normed[:, half:]
    rows = []
    for table in (first, second):
        ids = jnp.where(s == 0, table[16:24, :64], table[24:32, :64])
        wts = jnp.where(s == 0, table[32:40, :64], table[40:48, :64])
        rows.append(routing_rows(ids, wts, table[48:49, :]))
    table = jnp.concatenate(rows, axis=0)
    table = jnp.concatenate([table, jnp.zeros_like(table)], axis=1)
    table = jnp.concatenate([table, jnp.zeros_like(table)], axis=0)
    high[:, half:] = table.T[: hidden.shape[0], :].astype(BF)


def gather_body(zi, metas, blocks_low, blocks_high, layer, out, whole, emit):
    tok = 64
    half = whole.shape[1] // 2
    for i in range(LINE):
        whole[i * tok : (i + 1) * tok, :half] = blocks_low[i][...]
        whole[i * tok : (i + 1) * tok, half:] = blocks_high[i][:, :half]
    meta = metas()
    if emit is not None:
        emit[...] = meta
    rows = meta.astype(F32).T[layer * 32 : layer * 32 + 16, :]
    holder = rows[:8].astype(jnp.int32)
    rank = rows[8:].astype(jnp.int32)
    block = lax.broadcasted_iota(jnp.int32, holder.shape, 1) // tok
    place = ((holder // 32) * 4 + holder % 4) * (LINE * CAP) + block * CAP + rank
    slot = jnp.where((holder // 4) % LINE == zi, place, -1)
    total = out.shape[0]
    lanes = LINE * tok
    step = 128
    for r in range(0, total, step):
        index = lax.broadcasted_iota(jnp.int32, (step, lanes), 0) + r
        hit = index == slot[0:1, :]
        for k in range(1, 8):
            hit = jnp.logical_or(hit, index == slot[k : k + 1, :])
        pick = jnp.where(hit, 1.0, 0.0).astype(BF)
        out[r : r + step, :] = jnp.dot(pick, whole[...], preferred_element_type=F32).astype(BF)


def gather_first_kernel(zi, *refs):
    low, high = refs[:LINE], refs[LINE : 2 * LINE]
    out, emit, whole = refs[2 * LINE :]
    half = low[0].shape[1]
    metas = lambda: jnp.concatenate([h[:, half:] for h in high], axis=0)
    gather_body(zi[0], metas, low, high, 0, out, whole, emit)


def gather_later_kernel(zi, meta, *refs):
    low, high = refs[:LINE], refs[LINE : 2 * LINE]
    out, whole = refs[2 * LINE :]
    gather_body(zi[0], lambda: meta[...], low, high, 1, out, whole, None)


CHUNK = 256


def ffn_kernel(layer, sec, rows, ga, ua, da, gb, ub, db, out, wg, wu, wd, hidden, sems):
    own = sec[0] == layer
    chunks = wg.shape[1] // CHUNK

    def copies(g, u, d):
        found = []
        for n in range(chunks):
            part = pl.ds(n * CHUNK, CHUNK)
            found.append(pltpu.make_async_copy(g.at[:, part], wg.at[:, part], sems.at[2 * n]))
            found.append(pltpu.make_async_copy(u.at[:, part], wu.at[:, part], sems.at[2 * n + 1]))
        return found + [pltpu.make_async_copy(d, wd, sems.at[2 * chunks])]

    mine = copies(ga, ua, da)

    @pl.when(own)
    def _():
        for c in mine:
            c.start()

    @pl.when(jnp.logical_not(own))
    def _():
        for c in copies(gb, ub, db):
            c.start()

    dot = functools.partial(jnp.dot, preferred_element_type=F32)
    for n in range(chunks):
        part = slice(n * CHUNK, (n + 1) * CHUNK)
        mine[2 * n].wait()
        v = dot(rows[...], wg[:, part])
        mine[2 * n + 1].wait()
        hidden[:, part] = (v / (1.0 + jnp.exp(-v)) * dot(rows[...], wu[:, part])).astype(BF)
    mine[2 * chunks].wait()
    for n in range(0, out.shape[1], 512):
        part = slice(n, n + 512)
        out[:, part] = dot(hidden[...], wd[:, part]).astype(BF)


def combine_kernel(layer, zi, meta, rows, *outs):
    tok = 64
    half = rows.shape[1] // 2
    table = meta[:, layer * 32 : layer * 32 + 24].astype(F32)
    holder = table[:, :8].astype(jnp.int32)
    rank = table[:, 8:16].astype(jnp.int32)
    block = lax.broadcasted_iota(jnp.int32, holder.shape, 0) // tok
    place = ((holder // 32) * 4 + holder % 4) * (LINE * CAP) + block * CAP + rank
    slot = jnp.where((holder // 4) % LINE == zi[0], place, -1)
    total = rows.shape[0]
    for i in range(0, LINE, 2):
        part = slice(i * tok, (i + 2) * tok)
        index = lax.broadcasted_iota(jnp.int32, (2 * tok, total), 1)
        mix = jnp.zeros((2 * tok, total), F32)
        for k in range(8):
            mix = jnp.where(index == slot[part, k : k + 1], table[part, 16 + k : 17 + k], mix)
        mix = mix.astype(BF)
        for c in range(2):
            total_rows = jnp.dot(mix, rows[:, c * half : (c + 1) * half], preferred_element_type=F32)
            for b in range(2):
                outs[2 * (i + b) + c][...] = total_rows[b * tok : (b + 1) * tok].astype(BF)


def middle_kernel(sec, start, mine, theirs, *refs):
    f0, f1, b0, b1, p0, p1, kept, low, high = refs
    half = f0.shape[1]
    add = lambda x, y, z: x[...].astype(F32) + y[...].astype(F32) + z[...].astype(F32)
    hidden = start[...].astype(F32) + jnp.concatenate([add(p0, f0, b0), add(p1, f1, b1)], axis=1)
    hidden = hidden.astype(BF)
    kept[...] = hidden
    gain = gain_of(jnp.where(sec[0] == 0, theirs[:16, :], mine[:16, :]))
    normed = normalized(hidden.astype(F32), gain)
    low[...] = normed[:, :half]
    high[...] = normed[:, half:]


STAGGER = (14000, 10000)


def stagger_kernel(layer, sec, rows, out):
    @pl.when(sec[0] == layer)
    def _():
        pl.delay(STAGGER[layer])


def last_kernel(hidden, f0, f1, b0, b1, p0, p1, out):
    half = f0.shape[1]
    add = lambda x, y, z: x[...].astype(F32) + y[...].astype(F32) + z[...].astype(F32)
    out[:, :half] = (hidden[:, :half].astype(F32) + add(p0, f0, b0)).astype(BF)
    out[:, half:] = (hidden[:, half:].astype(F32) + add(p1, f1, b1)).astype(BF)


ORDER = (0, -1, 1, -2, 2, -3, 3, 4)


def line_gather(low, high):
    held = {0: (low, high)}
    ahead, behind = (low, high), (low, high)
    for step in (1, 2, 3):
        behind = tuple(shift(p, "z", 1, LINE) for p in behind)
        ahead = tuple(shift(p, "z", -1, LINE) for p in ahead)
        held[-step], held[step] = behind, ahead
    held[4] = (shift(behind[0], "z", 1, LINE), shift(ahead[1], "z", -1, LINE))
    return [held[o][0] for o in ORDER], [held[o][1] for o in ORDER]


def line_scatter(parts):
    low = {o: parts[2 * i] for i, o in enumerate(ORDER)}
    high = {o: parts[2 * i + 1] for i, o in enumerate(ORDER)}
    up = lambda p: shift(p, "z", 1, LINE)
    down = lambda p: shift(p, "z", -1, LINE)
    f0, b1 = up(low[4]), down(high[4])
    f0, b1 = up(low[3] + f0), down(high[-3] + b1)
    f1, b0 = up(high[3]), down(low[-3])
    for step in (2, 1):
        f0, f1 = up(low[step] + f0), up(high[step] + f1)
        b0, b1 = down(low[-step] + b0), down(high[-step] + b1)
    return f0, f1, b0, b1, low[0], high[0]


def plane_exchange(rows):
    parts = rows.reshape(16, rows.shape[0] // 16, rows.shape[1])
    return lax.all_to_all(parts, ("x", "y"), 0, 0, tiled=True).reshape(rows.shape)


def local(
    tokens, norm_gain, gate_weight, up_weight, down_weight, expert_place, expert_ids, route_weights
):
    section = lax.axis_index("section").astype(jnp.int32)[None]
    plane = lax.axis_index("z").astype(jnp.int32)[None]
    tok, width = tokens.shape[1], tokens.shape[2]
    half = width // 2
    slots = 16 * LINE * CAP
    lanes = LINE * tok
    ffe = gate_weight.shape[3]
    sds = jax.ShapeDtypeStruct
    anywhere = pl.BlockSpec(memory_space=HBM)

    swap = lambda v: shift(v, "section", 1, 2)
    ids = jnp.swapaxes(expert_ids[0], 1, 2)
    wts = jnp.swapaxes(route_weights[0], 1, 2)
    mine, start = pl.pallas_call(
        pack_kernel,
        out_shape=(sds((56, 128), F32), sds((tok, width), BF)),
        in_specs=[smem()] + [anywhere] * 5,
        out_specs=(vmem(), vmem()),
        scratch_shapes=[
            pltpu.VMEM((1, width), F32),
            pltpu.VMEM((1, 128), jnp.int32),
            pltpu.VMEM((2, 8, tok), jnp.int32),
            pltpu.VMEM((2, 8, tok), F32),
            pltpu.SemaphoreType.DMA((5,)),
        ],
        compiler_params=params(8),
        name="pack",
    )(section, *(pltpu.with_memory_space_constraint(v, HBM) for v in (tokens, norm_gain, expert_place, ids, wts)))
    theirs = swap(mine)

    low, high = pl.pallas_call(
        prepare_kernel,
        out_shape=(sds((tok, half), BF), sds((tok, half + 128), BF)),
        in_specs=[smem()] + [vmem()] * 3,
        out_specs=(vmem(), vmem()),
        compiler_params=params(16),
        name="prepare",
    )(section, start, mine, theirs)

    def experts(rows, layer, mats, mats_b):
        return pl.pallas_call(
            functools.partial(ffn_kernel, layer),
            out_shape=sds((slots, width), BF),
            in_specs=[smem(), vmem()] + [anywhere] * 3 + [pl.BlockSpec(memory_space=pl.ANY)] * 3,
            out_specs=vmem(),
            scratch_shapes=[
                pltpu.VMEM((width, ffe), BF),
                pltpu.VMEM((width, ffe), BF),
                pltpu.VMEM((ffe, width), BF),
                pltpu.VMEM((slots, ffe), BF),
                pltpu.SemaphoreType.DMA((2 * (ffe // CHUNK) + 1,)),
            ],
            compiler_params=params(32),
            name="experts",
        )(section, rows, *mats, *mats_b)

    def combine(rows, meta, layer):
        return pl.pallas_call(
            functools.partial(combine_kernel, layer),
            out_shape=[sds((tok, half), BF)] * (2 * LINE),
            in_specs=[smem(), vmem(), vmem()],
            out_specs=[vmem()] * (2 * LINE),
            compiler_params=params(20),
            name="combine",
        )(plane, meta, rows)

    def stagger(rows, layer):
        return pl.pallas_call(
            functools.partial(stagger_kernel, layer),
            out_shape=sds((slots, width), BF),
            in_specs=[smem(), vmem()],
            out_specs=vmem(),
            input_output_aliases={1: 0},
            compiler_params=params(8),
            name="stagger",
        )(section, rows)

    gather_scratch = [pltpu.VMEM((lanes, width), BF)]
    lows, highs = line_gather(low, high)
    outgoing, meta = pl.pallas_call(
        gather_first_kernel,
        out_shape=(sds((slots, width), BF), sds((lanes, 128), BF)),
        in_specs=[smem()] + [vmem()] * (2 * LINE),
        out_specs=(vmem(), vmem()),
        scratch_shapes=gather_scratch,
        compiler_params=params(20),
        name="spread",
    )(plane, *lows, *highs)

    mats = (gate_weight[0, 0], up_weight[0, 0], down_weight[0, 0])
    outgoing, mats = lax.optimization_barrier((outgoing, mats))
    mats_b = tuple(swap(m) for m in mats)
    mats = tuple(pltpu.with_memory_space_constraint(m, HBM) for m in mats)
    arrived = plane_exchange(stagger(outgoing, 0))
    returned = plane_exchange(experts(arrived, 0, mats, mats_b))
    sums = line_scatter(combine(returned, meta, 0))

    hidden, low, high = pl.pallas_call(
        middle_kernel,
        out_shape=(sds((tok, width), BF), sds((tok, half), BF), sds((tok, half), BF)),
        in_specs=[smem()] + [vmem()] * 9,
        out_specs=(vmem(), vmem(), vmem()),
        compiler_params=params(16),
        name="middle",
    )(section, start, mine, theirs, *sums)

    lows, highs = line_gather(low, high)
    outgoing = pl.pallas_call(
        gather_later_kernel,
        out_shape=sds((slots, width), BF),
        in_specs=[smem()] + [vmem()] * (2 * LINE + 1),
        out_specs=vmem(),
        scratch_shapes=gather_scratch,
        compiler_params=params(20),
        name="spread_later",
    )(plane, meta, *lows, *highs)
    returned = plane_exchange(experts(plane_exchange(stagger(outgoing, 1)), 1, mats, mats_b))
    sums = line_scatter(combine(returned, meta, 1))

    final = pl.pallas_call(
        last_kernel,
        out_shape=sds((tok, width), BF),
        in_specs=[vmem()] * 7,
        out_specs=vmem(),
        compiler_params=params(16),
        name="last",
    )(hidden, *sums)
    theirs = swap(final)
    mine_first = section[0] == 0
    return jnp.stack([jnp.where(mine_first, final, theirs), jnp.where(mine_first, theirs, final)])


def solution(mesh):
    fine = Mesh(mesh.devices.reshape(2, 4, 8, 4), ("section", "x", "z", "y"))
    line = ("x", "z", "y")
    in_specs = (
        P(None, line, None),
        P("section", None),
        P("section", line, None, None),
        P("section", line, None, None),
        P("section", line, None, None),
        P("section", None),
        P("section", None, line, None),
        P("section", None, line, None),
    )
    return jax.shard_map(
        local, mesh=fine, in_specs=in_specs, out_specs=P(None, line, None), check_vma=False
    )
```

```python
import functools

import jax
import jax.numpy as jnp
from jax import lax
from jax.experimental import pallas as pl
from jax.experimental.pallas import tpu as pltpu
from jax.sharding import Mesh, PartitionSpec as P

EPSILON = 1e-06
LINE = 8
CAP = 5
BF = jnp.bfloat16
F32 = jnp.float32
VMEM = pltpu.MemorySpace.VMEM
SMEM = pltpu.MemorySpace.SMEM
HBM = pltpu.MemorySpace.HBM


def vmem():
    return pl.BlockSpec(memory_space=VMEM)


def smem():
    return pl.BlockSpec(memory_space=SMEM)


def params(mib):
    return pltpu.CompilerParams(vmem_limit_bytes=mib << 20)


def shift(array, axis, by, size):
    return lax.ppermute(array, axis, [(i, (i + by) % size) for i in range(size)])


def normalized(hidden, gain):
    inverse = lax.rsqrt(jnp.mean(hidden * hidden, axis=-1, keepdims=True) + EPSILON)
    return (hidden * inverse * gain).astype(BF)


def routing_rows(ids, weights, place_row):
    tok = ids.shape[1]
    experts = lax.broadcasted_iota(jnp.int32, (128, tok), 0).astype(F32)
    hits = [(ids[k : k + 1, :] == experts).astype(F32) for k in range(8)]
    has = functools.reduce(jnp.add, hits)
    earlier = (
        lax.broadcasted_iota(jnp.int32, (tok, tok), 0) < lax.broadcasted_iota(jnp.int32, (tok, tok), 1)
    ).astype(F32)
    dot = functools.partial(jnp.dot, preferred_element_type=F32)
    before = dot(has.astype(BF), earlier.astype(BF))
    places = jnp.broadcast_to(place_row, (8, 128)).astype(BF)
    holders = [dot(places, h.astype(BF))[:1] for h in hits]
    positions = [jnp.sum(h * before, axis=0, keepdims=True) for h in hits]
    return jnp.concatenate(holders + positions + [weights, jnp.zeros_like(weights)], axis=0)


def pack_kernel(sec, tok, gain, place, ids, wts, table, hidden, gain_v, place_v, ids_v, wts_v, sems):
    copies = [
        pltpu.make_async_copy(gain, gain_v, sems.at[0]),
        pltpu.make_async_copy(place, place_v, sems.at[1]),
        pltpu.make_async_copy(ids, ids_v, sems.at[2]),
        pltpu.make_async_copy(wts, wts_v, sems.at[3]),
        pltpu.make_async_copy(tok.at[sec[0]], hidden, sems.at[4]),
    ]
    for c in copies:
        c.start()
    table[...] = jnp.zeros(table.shape, F32)
    for c in copies[:4]:
        c.wait()
    for i in range(16):
        table[i : i + 1, :] = gain_v[:, 128 * i : 128 * (i + 1)]
    for m in range(2):
        table[16 + 8 * m : 24 + 8 * m, :64] = ids_v[m].astype(F32)
        table[32 + 8 * m : 40 + 8 * m, :64] = wts_v[m]
    table[48:49, :] = place_v[...].astype(F32)
    copies[4].wait()


def gain_of(table):
    return jnp.concatenate([table[i : i + 1, :] for i in range(16)], axis=1)


def prepare_kernel(sec, hidden, mine, theirs, payload):
    s = sec[0]
    first = jnp.where(s == 0, mine[...], theirs[...])
    second = jnp.where(s == 0, theirs[...], mine[...])
    width = hidden.shape[1]
    payload[:, :width] = normalized(hidden[...].astype(F32), gain_of(first))
    rows = []
    for table in (first, second):
        ids = jnp.where(s == 0, table[16:24, :64], table[24:32, :64])
        wts = jnp.where(s == 0, table[32:40, :64], table[40:48, :64])
        rows.append(routing_rows(ids, wts, table[48:49, :]))
    table = jnp.concatenate(rows, axis=0)
    table = jnp.concatenate([table, jnp.zeros_like(table)], axis=1)
    table = jnp.concatenate([table, jnp.zeros_like(table)], axis=0)
    payload[:, width:] = table.T[: hidden.shape[0], :].astype(BF)


def assemble(whole, blocks):
    width = whole.shape[1]
    at = 0
    for b in blocks:
        whole[at : at + b.shape[0], :] = b[:, :width]
        at += b.shape[0]


def gather_body(zi, meta, blocks, layer, out, whole):
    tok = 64
    assemble(whole, blocks)
    rows = meta.astype(F32).T[layer * 32 : layer * 32 + 16, :]
    holder = rows[:8].astype(jnp.int32)
    rank = rows[8:].astype(jnp.int32)
    block = lax.broadcasted_iota(jnp.int32, holder.shape, 1) // tok
    place = ((holder // 32) * 4 + holder % 4) * (LINE * CAP) + block * CAP + rank
    slot = jnp.where((holder // 4) % LINE == zi, place, -1)
    lanes = LINE * tok
    step = 128
    for r in range(0, out.shape[0], step):
        index = lax.broadcasted_iota(jnp.int32, (step, lanes), 0) + r
        hit = index == slot[0:1, :]
        for k in range(1, 8):
            hit = jnp.logical_or(hit, index == slot[k : k + 1, :])
        pick = jnp.where(hit, 1.0, 0.0).astype(BF)
        out[r : r + step, :] = jnp.dot(pick, whole[...], preferred_element_type=F32).astype(BF)


def gather_first_kernel(zi, *refs):
    blocks = refs[: LINE + 1]
    out, emit, whole = refs[LINE + 1 :]
    width = whole.shape[1]
    meta = jnp.concatenate([b[:, width:] for b in blocks], axis=0)
    emit[...] = meta
    gather_body(zi[0], meta, blocks, 0, out, whole)


def gather_later_kernel(zi, meta, *refs):
    blocks = refs[: LINE + 1]
    out, whole = refs[LINE + 1 :]
    gather_body(zi[0], meta[...], blocks, 1, out, whole)


def ffn_kernel(layer, sec, rows, ga, ua, da, gb, ub, db, out, wg, wu, wd, gate, up, hidden, sems):
    own = sec[0] == layer
    half = wg.shape[0] // 2
    pieces = []
    for a, b, dst, lo, size in (
        (ga, gb, wg, 0, half),
        (ua, ub, wu, 0, half),
        (ga, gb, wg, half, half),
        (ua, ub, wu, half, half),
        (da, db, wd, 0, wd.shape[0]),
    ):
        part = pl.ds(lo, size)
        n = len(pieces)
        pieces.append(
            (
                pltpu.make_async_copy(a.at[part], dst.at[part], sems.at[n]),
                pltpu.make_async_copy(b.at[part], dst.at[part], sems.at[n]),
            )
        )

    @pl.when(own)
    def _():
        for mine, _ in pieces:
            mine.start()

    @pl.when(jnp.logical_not(own))
    def _():
        for _, theirs in pieces:
            theirs.start()

    dot = functools.partial(jnp.dot, preferred_element_type=F32)
    pieces[0][0].wait()
    gate[...] = dot(rows[:, :half], wg[:half])
    pieces[1][0].wait()
    up[...] = dot(rows[:, :half], wu[:half])
    pieces[2][0].wait()
    pieces[3][0].wait()
    step = rows.shape[0] // 2
    for r in range(0, rows.shape[0], step):
        part = slice(r, r + step)
        v = gate[part] + dot(rows[part, half:], wg[half:])
        u = up[part] + dot(rows[part, half:], wu[half:])
        hidden[part] = (v / (1.0 + jnp.exp(-v)) * u).astype(BF)
    pieces[4][0].wait()
    for r in range(0, rows.shape[0], step):
        part = slice(r, r + step)
        out[part] = dot(hidden[part], wd[...]).astype(BF)


def combine_kernel(layer, zi, meta, rows, *outs):
    tok = 64
    half = rows.shape[1] // 2
    table = meta[:, layer * 32 : layer * 32 + 24].astype(F32)
    holder = table[:, :8].astype(jnp.int32)
    rank = table[:, 8:16].astype(jnp.int32)
    block = lax.broadcasted_iota(jnp.int32, holder.shape, 0) // tok
    place = ((holder // 32) * 4 + holder % 4) * (LINE * CAP) + block * CAP + rank
    slot = jnp.where((holder // 4) % LINE == zi[0], place, -1)
    total = rows.shape[0]
    for i in range(0, LINE, 2):
        part = slice(i * tok, (i + 2) * tok)
        index = lax.broadcasted_iota(jnp.int32, (2 * tok, total), 1)
        mix = jnp.zeros((2 * tok, total), F32)
        for k in range(8):
            mix = jnp.where(index == slot[part, k : k + 1], table[part, 16 + k : 17 + k], mix)
        mix = mix.astype(BF)
        for c in range(2):
            columns = slice(c * half, (c + 1) * half)
            sums = jnp.dot(mix, rows[:, columns], preferred_element_type=F32).astype(BF)
            at = i * tok
            base = 0
            for o in outs:
                size = o.shape[0]
                if at <= base < at + 2 * tok:
                    o[:, columns] = sums[base - at : base - at + size]
                base += size


def with_sums(hidden, sums):
    return (hidden[...].astype(F32) + sum(x[...].astype(F32) for x in sums)).astype(BF)


def middle_kernel(sec, start, mine, theirs, f, b, p, kept, payload):
    hidden = with_sums(start, (p, f, b))
    kept[...] = hidden
    gain = gain_of(jnp.where(sec[0] == 0, theirs[:16, :], mine[:16, :]))
    payload[...] = normalized(hidden.astype(F32), gain)


def merge_kernel(top, came, own, far, out):
    tok = own.shape[0]
    half = tok // 2
    with_far = slice(0, half) if top else slice(half, tok)
    without = slice(half, tok) if top else slice(0, half)
    wide = lambda ref, rows: ref[rows, :].astype(F32)
    out[with_far, :] = (wide(came, with_far) + wide(own, with_far) + far[...].astype(F32)).astype(BF)
    out[without, :] = (wide(came, without) + wide(own, without)).astype(BF)


STAGGER = (14000, 10000)


def stagger_kernel(layer, sec, rows, out):
    @pl.when(sec[0] == layer)
    def _():
        pl.delay(STAGGER[layer])


def last_kernel(hidden, f, b, p, out):
    out[...] = with_sums(hidden, (p, f, b))


def line_gather(payload):
    behind, ahead = [payload], [payload]
    for _ in range(2):
        behind.append(shift(behind[-1], "z", 1, LINE))
        ahead.append(shift(ahead[-1], "z", -1, LINE))
    behind.append(shift(behind[2], "z", 1, LINE))
    ahead.append(shift(ahead[2], "z", -1, LINE))
    half = payload.shape[0] // 2
    far = (shift(behind[2][:half], "z", 2, LINE), shift(ahead[2][half:], "z", -2, LINE))
    return [payload, *(b for pair in zip(behind[1:], ahead[1:]) for b in pair), *far]


def merge(top, came, own, far):
    return pl.pallas_call(
        functools.partial(merge_kernel, top),
        out_shape=jax.ShapeDtypeStruct(own.shape, BF),
        in_specs=[vmem()] * 3,
        out_specs=vmem(),
        compiler_params=params(4),
        name="merge",
    )(came, own, far)


def line_scatter(parts):
    own, b1, a1, b2, a2, b3, a3, top, bottom = parts
    up = lambda p, by=1: shift(p, "z", by, LINE)
    f, b = up(a3), up(b3, -1)
    top, bottom = up(top, 2), up(bottom, -2)
    f, b = up(merge(True, f, a2, top)), up(merge(False, b, b2, bottom), -1)
    return up(a1 + f), up(b1 + b, -1), own


def plane_exchange(rows):
    parts = rows.reshape(16, rows.shape[0] // 16, rows.shape[1])
    return lax.all_to_all(parts, ("x", "y"), 0, 0, tiled=True).reshape(rows.shape)


def local(
    tokens, norm_gain, gate_weight, up_weight, down_weight, expert_place, expert_ids, route_weights
):
    section = lax.axis_index("section").astype(jnp.int32)[None]
    plane = lax.axis_index("z").astype(jnp.int32)[None]
    tok, width = tokens.shape[1], tokens.shape[2]
    slots = 16 * LINE * CAP
    lanes = LINE * tok
    ffe = gate_weight.shape[3]
    sds = jax.ShapeDtypeStruct
    anywhere = pl.BlockSpec(memory_space=HBM)

    swap = lambda v: shift(v, "section", 1, 2)
    ids = jnp.swapaxes(expert_ids[0], 1, 2)
    wts = jnp.swapaxes(route_weights[0], 1, 2)
    mine, start = pl.pallas_call(
        pack_kernel,
        out_shape=(sds((56, 128), F32), sds((tok, width), BF)),
        in_specs=[smem()] + [anywhere] * 5,
        out_specs=(vmem(), vmem()),
        scratch_shapes=[
            pltpu.VMEM((1, width), F32),
            pltpu.VMEM((1, 128), jnp.int32),
            pltpu.VMEM((2, 8, tok), jnp.int32),
            pltpu.VMEM((2, 8, tok), F32),
            pltpu.SemaphoreType.DMA((5,)),
        ],
        compiler_params=params(8),
        name="pack",
    )(section, *(pltpu.with_memory_space_constraint(v, HBM) for v in (tokens, norm_gain, expert_place, ids, wts)))
    theirs = swap(mine)

    payload = pl.pallas_call(
        prepare_kernel,
        out_shape=sds((tok, width + 128), BF),
        in_specs=[smem()] + [vmem()] * 3,
        out_specs=vmem(),
        compiler_params=params(16),
        name="prepare",
    )(section, start, mine, theirs)

    def experts(rows, layer, mats, mats_b):
        return pl.pallas_call(
            functools.partial(ffn_kernel, layer),
            out_shape=sds((slots, width), BF),
            in_specs=[smem(), vmem()] + [anywhere] * 3 + [pl.BlockSpec(memory_space=pl.ANY)] * 3,
            out_specs=vmem(),
            scratch_shapes=[
                pltpu.VMEM((width, ffe), BF),
                pltpu.VMEM((width, ffe), BF),
                pltpu.VMEM((ffe, width), BF),
                pltpu.VMEM((slots, ffe), F32),
                pltpu.VMEM((slots, ffe), F32),
                pltpu.VMEM((slots, ffe), BF),
                pltpu.SemaphoreType.DMA((5,)),
            ],
            compiler_params=params(32),
            name="experts",
        )(section, rows, *mats, *mats_b)

    def combine(rows, meta, layer):
        return pl.pallas_call(
            functools.partial(combine_kernel, layer),
            out_shape=[sds((tok, width), BF)] * (LINE - 1) + [sds((tok // 2, width), BF)] * 2,
            in_specs=[smem(), vmem(), vmem()],
            out_specs=[vmem()] * (LINE + 1),
            compiler_params=params(20),
            name="combine",
        )(plane, meta, rows)

    def stagger(rows, layer):
        return pl.pallas_call(
            functools.partial(stagger_kernel, layer),
            out_shape=sds((slots, width), BF),
            in_specs=[smem(), vmem()],
            out_specs=vmem(),
            input_output_aliases={1: 0},
            compiler_params=params(8),
            name="stagger",
        )(section, rows)

    gather_scratch = [pltpu.VMEM((lanes, width), BF)]
    outgoing, meta = pl.pallas_call(
        gather_first_kernel,
        out_shape=(sds((slots, width), BF), sds((lanes, 128), BF)),
        in_specs=[smem()] + [vmem()] * (LINE + 1),
        out_specs=(vmem(), vmem()),
        scratch_shapes=gather_scratch,
        compiler_params=params(20),
        name="spread",
    )(plane, *line_gather(payload))

    mats = (gate_weight[0, 0], up_weight[0, 0], down_weight[0, 0])
    outgoing, mats = lax.optimization_barrier((outgoing, mats))
    mats_b = tuple(swap(m) for m in mats)
    mats = tuple(pltpu.with_memory_space_constraint(m, HBM) for m in mats)
    arrived = plane_exchange(stagger(outgoing, 0))
    returned = plane_exchange(experts(arrived, 0, mats, mats_b))
    sums = line_scatter(combine(returned, meta, 0))

    hidden, payload = pl.pallas_call(
        middle_kernel,
        out_shape=(sds((tok, width), BF), sds((tok, width), BF)),
        in_specs=[smem()] + [vmem()] * 6,
        out_specs=(vmem(), vmem()),
        compiler_params=params(16),
        name="middle",
    )(section, start, mine, theirs, *sums)

    outgoing = pl.pallas_call(
        gather_later_kernel,
        out_shape=sds((slots, width), BF),
        in_specs=[smem()] + [vmem()] * (LINE + 2),
        out_specs=vmem(),
        scratch_shapes=gather_scratch,
        compiler_params=params(20),
        name="spread_later",
    )(plane, meta, *line_gather(payload))
    returned = plane_exchange(experts(plane_exchange(stagger(outgoing, 1)), 1, mats, mats_b))
    sums = line_scatter(combine(returned, meta, 1))

    final = pl.pallas_call(
        last_kernel,
        out_shape=sds((tok, width), BF),
        in_specs=[vmem()] * 4,
        out_specs=vmem(),
        compiler_params=params(16),
        name="last",
    )(hidden, *sums)
    theirs = swap(final)
    mine_first = section[0] == 0
    return jnp.stack([jnp.where(mine_first, final, theirs), jnp.where(mine_first, theirs, final)])


def solution(mesh):
    fine = Mesh(mesh.devices.reshape(2, 4, 8, 4), ("section", "x", "z", "y"))
    line = ("x", "z", "y")
    in_specs = (
        P(None, line, None),
        P("section", None),
        P("section", line, None, None),
        P("section", line, None, None),
        P("section", line, None, None),
        P("section", None),
        P("section", None, line, None),
        P("section", None, line, None),
    )
    return jax.shard_map(
        local, mesh=fine, in_specs=in_specs, out_specs=P(None, line, None), check_vma=False
    )
```

```python
import functools

import jax
import jax.numpy as jnp
from jax import lax
from jax.experimental import pallas as pl
from jax.experimental.pallas import tpu as pltpu
from jax.sharding import Mesh, PartitionSpec as P

EPSILON = 1e-06
LINE = 8
CAP = 5
BF = jnp.bfloat16
F32 = jnp.float32
VMEM = pltpu.MemorySpace.VMEM
SMEM = pltpu.MemorySpace.SMEM
HBM = pltpu.MemorySpace.HBM


def vmem():
    return pl.BlockSpec(memory_space=VMEM)


def smem():
    return pl.BlockSpec(memory_space=SMEM)


def params(mib):
    return pltpu.CompilerParams(vmem_limit_bytes=mib << 20)


def shift(array, axis, by, size):
    return lax.ppermute(array, axis, [(i, (i + by) % size) for i in range(size)])


def normalized(hidden, gain):
    inverse = lax.rsqrt(jnp.mean(hidden * hidden, axis=-1, keepdims=True) + EPSILON)
    return (hidden * inverse * gain).astype(BF)


def routing_rows(ids, weights, place_row):
    tok = ids.shape[1]
    experts = lax.broadcasted_iota(jnp.int32, (128, tok), 0).astype(F32)
    hits = [(ids[k : k + 1, :] == experts).astype(F32) for k in range(8)]
    has = functools.reduce(jnp.add, hits)
    earlier = (
        lax.broadcasted_iota(jnp.int32, (tok, tok), 0) < lax.broadcasted_iota(jnp.int32, (tok, tok), 1)
    ).astype(F32)
    dot = functools.partial(jnp.dot, preferred_element_type=F32)
    before = dot(has.astype(BF), earlier.astype(BF))
    places = jnp.broadcast_to(place_row, (8, 128)).astype(BF)
    holders = [dot(places, h.astype(BF))[:1] for h in hits]
    positions = [jnp.sum(h * before, axis=0, keepdims=True) for h in hits]
    return jnp.concatenate(holders + positions + [weights, jnp.zeros_like(weights)], axis=0)


def pack_kernel(sec, tok, gain, place, ids, wts, table, hidden, gain_v, place_v, ids_v, wts_v, sems):
    copies = [
        pltpu.make_async_copy(gain, gain_v, sems.at[0]),
        pltpu.make_async_copy(place, place_v, sems.at[1]),
        pltpu.make_async_copy(ids, ids_v, sems.at[2]),
        pltpu.make_async_copy(wts, wts_v, sems.at[3]),
        pltpu.make_async_copy(tok.at[sec[0]], hidden, sems.at[4]),
    ]
    for c in copies:
        c.start()
    table[...] = jnp.zeros(table.shape, F32)
    for c in copies[:4]:
        c.wait()
    for i in range(16):
        table[i : i + 1, :] = gain_v[:, 128 * i : 128 * (i + 1)]
    for m in range(2):
        table[16 + 8 * m : 24 + 8 * m, :64] = ids_v[m].astype(F32)
        table[32 + 8 * m : 40 + 8 * m, :64] = wts_v[m]
    table[48:49, :] = place_v[...].astype(F32)
    copies[4].wait()


def gain_of(table):
    return jnp.concatenate([table[i : i + 1, :] for i in range(16)], axis=1)


def prepare_kernel(sec, hidden, mine, theirs, low, high):
    s = sec[0]
    first = jnp.where(s == 0, mine[...], theirs[...])
    second = jnp.where(s == 0, theirs[...], mine[...])
    half = hidden.shape[1] // 2
    normed = normalized(hidden[...].astype(F32), gain_of(first))
    low[...] = normed[:, :half]
    high[:, :half] = normed[:, half:]
    rows = []
    for table in (first, second):
        ids = jnp.where(s == 0, table[16:24, :64], table[24:32, :64])
        wts = jnp.where(s == 0, table[32:40, :64], table[40:48, :64])
        rows.append(routing_rows(ids, wts, table[48:49, :]))
    table = jnp.concatenate(rows, axis=0)
    table = jnp.concatenate([table, jnp.zeros_like(table)], axis=1)
    table = jnp.concatenate([table, jnp.zeros_like(table)], axis=0)
    high[:, half:] = table.T[: hidden.shape[0], :].astype(BF)


def gather_body(zi, metas, blocks_low, blocks_high, layer, out, whole, emit):
    tok = 64
    half = whole.shape[1] // 2
    for i in range(LINE):
        whole[i * tok : (i + 1) * tok, :half] = blocks_low[i][...]
        whole[i * tok : (i + 1) * tok, half:] = blocks_high[i][:, :half]
    meta = metas()
    if emit is not None:
        emit[...] = meta
    rows = meta.astype(F32).T[layer * 32 : layer * 32 + 16, :]
    holder = rows[:8].astype(jnp.int32)
    rank = rows[8:].astype(jnp.int32)
    block = lax.broadcasted_iota(jnp.int32, holder.shape, 1) // tok
    place = ((holder // 32) * 4 + holder % 4) * (LINE * CAP) + block * CAP + rank
    slot = jnp.where((holder // 4) % LINE == zi, place, -1)
    total = out.shape[0]
    lanes = LINE * tok
    step = 128
    for r in range(0, total, step):
        index = lax.broadcasted_iota(jnp.int32, (step, lanes), 0) + r
        hit = index == slot[0:1, :]
        for k in range(1, 8):
            hit = jnp.logical_or(hit, index == slot[k : k + 1, :])
        pick = jnp.where(hit, 1.0, 0.0).astype(BF)
        out[r : r + step, :] = jnp.dot(pick, whole[...], preferred_element_type=F32).astype(BF)


def gather_first_kernel(zi, *refs):
    low, high = refs[:LINE], refs[LINE : 2 * LINE]
    out, emit, whole = refs[2 * LINE :]
    half = low[0].shape[1]
    metas = lambda: jnp.concatenate([h[:, half:] for h in high], axis=0)
    gather_body(zi[0], metas, low, high, 0, out, whole, emit)


def gather_later_kernel(zi, meta, *refs):
    low, high = refs[:LINE], refs[LINE : 2 * LINE]
    out, whole = refs[2 * LINE :]
    gather_body(zi[0], lambda: meta[...], low, high, 1, out, whole, None)


def ffn_kernel(layer, sec, rows, ga, ua, da, gb, ub, db, out, wg, wu, wd, gate, up, hidden, sems):
    own = sec[0] == layer
    half = wg.shape[0] // 2
    pieces = []
    for a, b, dst, lo, size in (
        (ga, gb, wg, 0, half),
        (ua, ub, wu, 0, half),
        (ga, gb, wg, half, half),
        (ua, ub, wu, half, half),
        (da, db, wd, 0, wd.shape[0]),
    ):
        part = pl.ds(lo, size)
        n = len(pieces)
        pieces.append(
            (
                pltpu.make_async_copy(a.at[part], dst.at[part], sems.at[n]),
                pltpu.make_async_copy(b.at[part], dst.at[part], sems.at[n]),
            )
        )

    @pl.when(own)
    def _():
        for mine, _ in pieces:
            mine.start()

    @pl.when(jnp.logical_not(own))
    def _():
        for _, theirs in pieces:
            theirs.start()

    dot = functools.partial(jnp.dot, preferred_element_type=F32)
    pieces[0][0].wait()
    gate[...] = dot(rows[:, :half], wg[:half])
    pieces[1][0].wait()
    up[...] = dot(rows[:, :half], wu[:half])
    pieces[2][0].wait()
    pieces[3][0].wait()
    step = rows.shape[0] // 2
    for r in range(0, rows.shape[0], step):
        part = slice(r, r + step)
        v = gate[part] + dot(rows[part, half:], wg[half:])
        u = up[part] + dot(rows[part, half:], wu[half:])
        hidden[part] = (v / (1.0 + jnp.exp(-v)) * u).astype(BF)
    pieces[4][0].wait()
    for r in range(0, rows.shape[0], step):
        part = slice(r, r + step)
        out[part] = dot(hidden[part], wd[...]).astype(BF)


def combine_kernel(layer, zi, meta, rows, *outs):
    tok = 64
    half = rows.shape[1] // 2
    table = meta[:, layer * 32 : layer * 32 + 24].astype(F32)
    holder = table[:, :8].astype(jnp.int32)
    rank = table[:, 8:16].astype(jnp.int32)
    block = lax.broadcasted_iota(jnp.int32, holder.shape, 0) // tok
    place = ((holder // 32) * 4 + holder % 4) * (LINE * CAP) + block * CAP + rank
    slot = jnp.where((holder // 4) % LINE == zi[0], place, -1)
    total = rows.shape[0]
    for i in range(0, LINE, 2):
        part = slice(i * tok, (i + 2) * tok)
        index = lax.broadcasted_iota(jnp.int32, (2 * tok, total), 1)
        mix = jnp.zeros((2 * tok, total), F32)
        for k in range(8):
            mix = jnp.where(index == slot[part, k : k + 1], table[part, 16 + k : 17 + k], mix)
        mix = mix.astype(BF)
        for c in range(2):
            columns = slice(c * half, (c + 1) * half)
            sums = jnp.dot(mix, rows[:, columns], preferred_element_type=F32).astype(BF)
            at = i * tok
            base = 0
            for o in outs:
                size = o.shape[0]
                if at <= base < at + 2 * tok:
                    o[:, columns] = sums[base - at : base - at + size]
                base += size


def with_sums(hidden, sums):
    return (hidden[...].astype(F32) + sum(x[...].astype(F32) for x in sums)).astype(BF)


def middle_kernel(sec, start, mine, theirs, f, b, p, kept, low, high):
    hidden = with_sums(start, (p, f, b))
    kept[...] = hidden
    gain = gain_of(jnp.where(sec[0] == 0, theirs[:16, :], mine[:16, :]))
    normed = normalized(hidden.astype(F32), gain)
    half = low.shape[1]
    low[...] = normed[:, :half]
    high[...] = normed[:, half:]


def merge_kernel(top, came, own, far, out):
    tok = own.shape[0]
    half = tok // 2
    with_far = slice(0, half) if top else slice(half, tok)
    without = slice(half, tok) if top else slice(0, half)
    wide = lambda ref, rows: ref[rows, :].astype(F32)
    out[with_far, :] = (wide(came, with_far) + wide(own, with_far) + far[...].astype(F32)).astype(BF)
    out[without, :] = (wide(came, without) + wide(own, without)).astype(BF)


STAGGER = (13000, 10000)


def stagger_kernel(layer, sec, rows, out):
    @pl.when(sec[0] == layer)
    def _():
        pl.delay(STAGGER[layer])


def last_kernel(hidden, f, b, p, out):
    out[...] = with_sums(hidden, (p, f, b))


ORDER = (0, -1, 1, -2, 2, -3, 3, 4)


def line_gather(low, high):
    held = {0: (low, high)}
    ahead, behind = (low, high), (low, high)
    for step in (1, 2, 3):
        if step == 3:
            two_behind, two_ahead = behind, ahead
        behind = tuple(shift(p, "z", 1, LINE) for p in behind)
        ahead = tuple(shift(p, "z", -1, LINE) for p in ahead)
        held[-step], held[step] = behind, ahead
    held[4] = (shift(two_behind[0], "z", 2, LINE), shift(two_ahead[1], "z", -2, LINE))
    return [held[o][0] for o in ORDER], [held[o][1] for o in ORDER]


def merge(top, came, own, far):
    return pl.pallas_call(
        functools.partial(merge_kernel, top),
        out_shape=jax.ShapeDtypeStruct(own.shape, BF),
        in_specs=[vmem()] * 3,
        out_specs=vmem(),
        compiler_params=params(4),
        name="merge",
    )(came, own, far)


def line_scatter(parts):
    own, b1, a1, b2, a2, b3, a3, top, bottom = parts
    up = lambda p, by=1: shift(p, "z", by, LINE)
    f, b = up(a3), up(b3, -1)
    top, bottom = up(top, 2), up(bottom, -2)
    f, b = up(merge(True, f, a2, top)), up(merge(False, b, b2, bottom), -1)
    return up(a1 + f), up(b1 + b, -1), own


def plane_exchange(rows):
    parts = rows.reshape(16, rows.shape[0] // 16, rows.shape[1])
    return lax.all_to_all(parts, ("x", "y"), 0, 0, tiled=True).reshape(rows.shape)


def local(
    tokens, norm_gain, gate_weight, up_weight, down_weight, expert_place, expert_ids, route_weights
):
    section = lax.axis_index("section").astype(jnp.int32)[None]
    plane = lax.axis_index("z").astype(jnp.int32)[None]
    tok, width = tokens.shape[1], tokens.shape[2]
    half = width // 2
    slots = 16 * LINE * CAP
    lanes = LINE * tok
    ffe = gate_weight.shape[3]
    sds = jax.ShapeDtypeStruct
    anywhere = pl.BlockSpec(memory_space=HBM)

    swap = lambda v: shift(v, "section", 1, 2)
    ids = jnp.swapaxes(expert_ids[0], 1, 2)
    wts = jnp.swapaxes(route_weights[0], 1, 2)
    mine, start = pl.pallas_call(
        pack_kernel,
        out_shape=(sds((56, 128), F32), sds((tok, width), BF)),
        in_specs=[smem()] + [anywhere] * 5,
        out_specs=(vmem(), vmem()),
        scratch_shapes=[
            pltpu.VMEM((1, width), F32),
            pltpu.VMEM((1, 128), jnp.int32),
            pltpu.VMEM((2, 8, tok), jnp.int32),
            pltpu.VMEM((2, 8, tok), F32),
            pltpu.SemaphoreType.DMA((5,)),
        ],
        compiler_params=params(8),
        name="pack",
    )(section, *(pltpu.with_memory_space_constraint(v, HBM) for v in (tokens, norm_gain, expert_place, ids, wts)))
    theirs = swap(mine)

    low, high = pl.pallas_call(
        prepare_kernel,
        out_shape=(sds((tok, half), BF), sds((tok, half + 128), BF)),
        in_specs=[smem()] + [vmem()] * 3,
        out_specs=(vmem(), vmem()),
        compiler_params=params(16),
        name="prepare",
    )(section, start, mine, theirs)

    def experts(rows, layer, mats, mats_b):
        return pl.pallas_call(
            functools.partial(ffn_kernel, layer),
            out_shape=sds((slots, width), BF),
            in_specs=[smem(), vmem()] + [anywhere] * 3 + [pl.BlockSpec(memory_space=pl.ANY)] * 3,
            out_specs=vmem(),
            scratch_shapes=[
                pltpu.VMEM((width, ffe), BF),
                pltpu.VMEM((width, ffe), BF),
                pltpu.VMEM((ffe, width), BF),
                pltpu.VMEM((slots, ffe), F32),
                pltpu.VMEM((slots, ffe), F32),
                pltpu.VMEM((slots, ffe), BF),
                pltpu.SemaphoreType.DMA((5,)),
            ],
            compiler_params=params(32),
            name="experts",
        )(section, rows, *mats, *mats_b)

    def combine(rows, meta, layer):
        return pl.pallas_call(
            functools.partial(combine_kernel, layer),
            out_shape=[sds((tok, width), BF)] * (LINE - 1) + [sds((tok // 2, width), BF)] * 2,
            in_specs=[smem(), vmem(), vmem()],
            out_specs=[vmem()] * (LINE + 1),
            compiler_params=params(20),
            name="combine",
        )(plane, meta, rows)

    def stagger(rows, layer):
        return pl.pallas_call(
            functools.partial(stagger_kernel, layer),
            out_shape=sds((slots, width), BF),
            in_specs=[smem(), vmem()],
            out_specs=vmem(),
            input_output_aliases={1: 0},
            compiler_params=params(8),
            name="stagger",
        )(section, rows)

    gather_scratch = [pltpu.VMEM((lanes, width), BF)]
    lows, highs = line_gather(low, high)
    outgoing, meta = pl.pallas_call(
        gather_first_kernel,
        out_shape=(sds((slots, width), BF), sds((lanes, 128), BF)),
        in_specs=[smem()] + [vmem()] * (2 * LINE),
        out_specs=(vmem(), vmem()),
        scratch_shapes=gather_scratch,
        compiler_params=params(20),
        name="spread",
    )(plane, *lows, *highs)

    mats = (gate_weight[0, 0], up_weight[0, 0], down_weight[0, 0])
    outgoing, mats = lax.optimization_barrier((outgoing, mats))
    mats_b = tuple(swap(m) for m in mats)
    mats = tuple(pltpu.with_memory_space_constraint(m, HBM) for m in mats)
    arrived = plane_exchange(stagger(outgoing, 0))
    returned = plane_exchange(experts(arrived, 0, mats, mats_b))
    sums = line_scatter(combine(returned, meta, 0))

    hidden, low, high = pl.pallas_call(
        middle_kernel,
        out_shape=(sds((tok, width), BF), sds((tok, half), BF), sds((tok, half), BF)),
        in_specs=[smem()] + [vmem()] * 6,
        out_specs=(vmem(), vmem(), vmem()),
        compiler_params=params(16),
        name="middle",
    )(section, start, mine, theirs, *sums)

    lows, highs = line_gather(low, high)
    outgoing = pl.pallas_call(
        gather_later_kernel,
        out_shape=sds((slots, width), BF),
        in_specs=[smem()] + [vmem()] * (2 * LINE + 1),
        out_specs=vmem(),
        scratch_shapes=gather_scratch,
        compiler_params=params(20),
        name="spread_later",
    )(plane, meta, *lows, *highs)
    returned = plane_exchange(experts(plane_exchange(stagger(outgoing, 1)), 1, mats, mats_b))
    sums = line_scatter(combine(returned, meta, 1))

    final = pl.pallas_call(
        last_kernel,
        out_shape=sds((tok, width), BF),
        in_specs=[vmem()] * 4,
        out_specs=vmem(),
        compiler_params=params(16),
        name="last",
    )(hidden, *sums)
    theirs = swap(final)
    mine_first = section[0] == 0
    return jnp.stack([jnp.where(mine_first, final, theirs), jnp.where(mine_first, theirs, final)])


def solution(mesh):
    fine = Mesh(mesh.devices.reshape(2, 4, 8, 4), ("section", "x", "z", "y"))
    line = ("x", "z", "y")
    in_specs = (
        P(None, line, None),
        P("section", None),
        P("section", line, None, None),
        P("section", line, None, None),
        P("section", line, None, None),
        P("section", None),
        P("section", None, line, None),
        P("section", None, line, None),
    )
    return jax.shard_map(
        local, mesh=fine, in_specs=in_specs, out_specs=P(None, line, None), check_vma=False
    )
```

```python
import functools

import jax
import jax.numpy as jnp
from jax import lax
from jax.experimental import pallas as pl
from jax.experimental.pallas import tpu as pltpu
from jax.sharding import Mesh, PartitionSpec as P

EPSILON = 1e-06
LINE = 8
CAP = 5
BF = jnp.bfloat16
F32 = jnp.float32
VMEM = pltpu.MemorySpace.VMEM
SMEM = pltpu.MemorySpace.SMEM
HBM = pltpu.MemorySpace.HBM


def vmem():
    return pl.BlockSpec(memory_space=VMEM)


def smem():
    return pl.BlockSpec(memory_space=SMEM)


def params(mib):
    return pltpu.CompilerParams(vmem_limit_bytes=mib << 20)


def shift(array, axis, by, size):
    return lax.ppermute(array, axis, [(i, (i + by) % size) for i in range(size)])


def normalized(hidden, gain):
    inverse = lax.rsqrt(jnp.mean(hidden * hidden, axis=-1, keepdims=True) + EPSILON)
    return (hidden * inverse * gain).astype(BF)


def routing_rows(ids, weights, place_row):
    tok = ids.shape[1]
    experts = lax.broadcasted_iota(jnp.int32, (128, tok), 0).astype(F32)
    hits = [(ids[k : k + 1, :] == experts).astype(F32) for k in range(8)]
    has = functools.reduce(jnp.add, hits)
    earlier = (
        lax.broadcasted_iota(jnp.int32, (tok, tok), 0) < lax.broadcasted_iota(jnp.int32, (tok, tok), 1)
    ).astype(F32)
    dot = functools.partial(jnp.dot, preferred_element_type=F32)
    before = dot(has.astype(BF), earlier.astype(BF))
    places = jnp.broadcast_to(place_row, (8, 128)).astype(BF)
    holders = [dot(places, h.astype(BF))[:1] for h in hits]
    positions = [jnp.sum(h * before, axis=0, keepdims=True) for h in hits]
    return jnp.concatenate(holders + positions + [weights, jnp.zeros_like(weights)], axis=0)


def pack_kernel(sec, tok, gain, place, ids, wts, table, hidden, gain_v, place_v, ids_v, wts_v, sems):
    copies = [
        pltpu.make_async_copy(gain, gain_v, sems.at[0]),
        pltpu.make_async_copy(place, place_v, sems.at[1]),
        pltpu.make_async_copy(ids, ids_v, sems.at[2]),
        pltpu.make_async_copy(wts, wts_v, sems.at[3]),
        pltpu.make_async_copy(tok.at[sec[0]], hidden, sems.at[4]),
    ]
    for c in copies:
        c.start()
    table[...] = jnp.zeros(table.shape, F32)
    for c in copies[:4]:
        c.wait()
    for i in range(16):
        table[i : i + 1, :] = gain_v[:, 128 * i : 128 * (i + 1)]
    for m in range(2):
        table[16 + 8 * m : 24 + 8 * m, :64] = ids_v[m].astype(F32)
        table[32 + 8 * m : 40 + 8 * m, :64] = wts_v[m]
    table[48:49, :] = place_v[...].astype(F32)
    copies[4].wait()


def gain_of(table):
    return jnp.concatenate([table[i : i + 1, :] for i in range(16)], axis=1)


def prepare_kernel(sec, hidden, mine, theirs, low, high):
    s = sec[0]
    first = jnp.where(s == 0, mine[...], theirs[...])
    second = jnp.where(s == 0, theirs[...], mine[...])
    half = hidden.shape[1] // 2
    normed = normalized(hidden[...].astype(F32), gain_of(first))
    low[...] = normed[:, :half]
    high[:, :half] = normed[:, half:]
    rows = []
    for table in (first, second):
        ids = jnp.where(s == 0, table[16:24, :64], table[24:32, :64])
        wts = jnp.where(s == 0, table[32:40, :64], table[40:48, :64])
        rows.append(routing_rows(ids, wts, table[48:49, :]))
    table = jnp.concatenate(rows, axis=0)
    table = jnp.concatenate([table, jnp.zeros_like(table)], axis=1)
    table = jnp.concatenate([table, jnp.zeros_like(table)], axis=0)
    high[:, half:] = table.T[: hidden.shape[0], :].astype(BF)


def gather_body(zi, metas, blocks_low, blocks_high, layer, out, whole, emit):
    tok = 64
    half = whole.shape[1] // 2
    for i in range(LINE):
        whole[i * tok : (i + 1) * tok, :half] = blocks_low[i][...]
        whole[i * tok : (i + 1) * tok, half:] = blocks_high[i][:, :half]
    meta = metas()
    if emit is not None:
        emit[...] = meta
    rows = meta.astype(F32).T[layer * 32 : layer * 32 + 16, :]
    holder = rows[:8].astype(jnp.int32)
    rank = rows[8:].astype(jnp.int32)
    block = lax.broadcasted_iota(jnp.int32, holder.shape, 1) // tok
    place = ((holder // 32) * 4 + holder % 4) * (LINE * CAP) + block * CAP + rank
    slot = jnp.where((holder // 4) % LINE == zi, place, -1)
    total = out.shape[0]
    lanes = LINE * tok
    step = 128
    for r in range(0, total, step):
        index = lax.broadcasted_iota(jnp.int32, (step, lanes), 0) + r
        hit = index == slot[0:1, :]
        for k in range(1, 8):
            hit = jnp.logical_or(hit, index == slot[k : k + 1, :])
        pick = jnp.where(hit, 1.0, 0.0).astype(BF)
        out[r : r + step, :] = jnp.dot(pick, whole[...], preferred_element_type=F32).astype(BF)


def gather_first_kernel(zi, *refs):
    low, high = refs[:LINE], refs[LINE : 2 * LINE]
    out, emit, whole = refs[2 * LINE :]
    half = low[0].shape[1]
    metas = lambda: jnp.concatenate([h[:, half:] for h in high], axis=0)
    gather_body(zi[0], metas, low, high, 0, out, whole, emit)


def gather_later_kernel(zi, meta, *refs):
    low, high = refs[:LINE], refs[LINE : 2 * LINE]
    out, whole = refs[2 * LINE :]
    gather_body(zi[0], lambda: meta[...], low, high, 1, out, whole, None)


def ffn_kernel(layer, sec, rows, ga, ua, da, gb, ub, db, out, wg, wu, wd, gate, up, hidden, sems):
    own = sec[0] == layer
    half = wg.shape[0] // 2
    pieces = []
    for a, b, dst, lo, size in (
        (ga, gb, wg, 0, half),
        (ua, ub, wu, 0, half),
        (ga, gb, wg, half, half),
        (ua, ub, wu, half, half),
        (da, db, wd, 0, wd.shape[0]),
    ):
        part = pl.ds(lo, size)
        n = len(pieces)
        pieces.append(
            (
                pltpu.make_async_copy(a.at[part], dst.at[part], sems.at[n]),
                pltpu.make_async_copy(b.at[part], dst.at[part], sems.at[n]),
            )
        )

    @pl.when(own)
    def _():
        for mine, _ in pieces:
            mine.start()

    @pl.when(jnp.logical_not(own))
    def _():
        for _, theirs in pieces:
            theirs.start()

    dot = functools.partial(jnp.dot, preferred_element_type=F32)
    pieces[0][0].wait()
    gate[...] = dot(rows[:, :half], wg[:half])
    pieces[1][0].wait()
    up[...] = dot(rows[:, :half], wu[:half])
    pieces[2][0].wait()
    pieces[3][0].wait()
    step = rows.shape[0] // 2
    for r in range(0, rows.shape[0], step):
        part = slice(r, r + step)
        v = gate[part] + dot(rows[part, half:], wg[half:])
        u = up[part] + dot(rows[part, half:], wu[half:])
        hidden[part] = (v / (1.0 + jnp.exp(-v)) * u).astype(BF)
    pieces[4][0].wait()
    for r in range(0, rows.shape[0], step):
        part = slice(r, r + step)
        out[part] = dot(hidden[part], wd[...]).astype(BF)


def combine_kernel(layer, zi, meta, rows, *outs):
    tok = 64
    half = rows.shape[1] // 2
    table = meta[:, layer * 32 : layer * 32 + 24].astype(F32)
    holder = table[:, :8].astype(jnp.int32)
    rank = table[:, 8:16].astype(jnp.int32)
    block = lax.broadcasted_iota(jnp.int32, holder.shape, 0) // tok
    place = ((holder // 32) * 4 + holder % 4) * (LINE * CAP) + block * CAP + rank
    slot = jnp.where((holder // 4) % LINE == zi[0], place, -1)
    total = rows.shape[0]
    for i in range(0, LINE, 2):
        part = slice(i * tok, (i + 2) * tok)
        index = lax.broadcasted_iota(jnp.int32, (2 * tok, total), 1)
        mix = jnp.zeros((2 * tok, total), F32)
        for k in range(8):
            mix = jnp.where(index == slot[part, k : k + 1], table[part, 16 + k : 17 + k], mix)
        mix = mix.astype(BF)
        for c in range(2):
            total_rows = jnp.dot(mix, rows[:, c * half : (c + 1) * half], preferred_element_type=F32)
            for b in range(2):
                outs[2 * (i + b) + c][...] = total_rows[b * tok : (b + 1) * tok].astype(BF)


def middle_kernel(sec, start, mine, theirs, *refs):
    f0, f1, b0, b1, p0, p1, kept, low, high = refs
    half = f0.shape[1]
    add = lambda x, y, z: x[...].astype(F32) + y[...].astype(F32) + z[...].astype(F32)
    hidden = start[...].astype(F32) + jnp.concatenate([add(p0, f0, b0), add(p1, f1, b1)], axis=1)
    hidden = hidden.astype(BF)
    kept[...] = hidden
    gain = gain_of(jnp.where(sec[0] == 0, theirs[:16, :], mine[:16, :]))
    normed = normalized(hidden.astype(F32), gain)
    low[...] = normed[:, :half]
    high[...] = normed[:, half:]


STAGGER = (13000, 10000)


def stagger_kernel(layer, sec, rows, out):
    @pl.when(sec[0] == layer)
    def _():
        pl.delay(STAGGER[layer])


def last_kernel(hidden, f0, f1, b0, b1, p0, p1, out):
    half = f0.shape[1]
    add = lambda x, y, z: x[...].astype(F32) + y[...].astype(F32) + z[...].astype(F32)
    out[:, :half] = (hidden[:, :half].astype(F32) + add(p0, f0, b0)).astype(BF)
    out[:, half:] = (hidden[:, half:].astype(F32) + add(p1, f1, b1)).astype(BF)


ORDER = (0, -1, 1, -2, 2, -3, 3, 4)


def line_gather(low, high):
    held = {0: (low, high)}
    ahead, behind = (low, high), (low, high)
    for step in (1, 2, 3):
        behind = tuple(shift(p, "z", 1, LINE) for p in behind)
        ahead = tuple(shift(p, "z", -1, LINE) for p in ahead)
        held[-step], held[step] = behind, ahead
    held[4] = (shift(behind[0], "z", 1, LINE), shift(ahead[1], "z", -1, LINE))
    return [held[o][0] for o in ORDER], [held[o][1] for o in ORDER]


def line_scatter(parts):
    low = {o: parts[2 * i] for i, o in enumerate(ORDER)}
    high = {o: parts[2 * i + 1] for i, o in enumerate(ORDER)}
    up = lambda p: shift(p, "z", 1, LINE)
    down = lambda p: shift(p, "z", -1, LINE)
    f0, b1 = up(low[4]), down(high[4])
    f0, b1 = up(low[3] + f0), down(high[-3] + b1)
    f1, b0 = up(high[3]), down(low[-3])
    for step in (2, 1):
        f0, f1 = up(low[step] + f0), up(high[step] + f1)
        b0, b1 = down(low[-step] + b0), down(high[-step] + b1)
    return f0, f1, b0, b1, low[0], high[0]


def plane_exchange(rows):
    parts = rows.reshape(16, rows.shape[0] // 16, rows.shape[1])
    return lax.all_to_all(parts, ("x", "y"), 0, 0, tiled=True).reshape(rows.shape)


def local(
    tokens, norm_gain, gate_weight, up_weight, down_weight, expert_place, expert_ids, route_weights
):
    section = lax.axis_index("section").astype(jnp.int32)[None]
    plane = lax.axis_index("z").astype(jnp.int32)[None]
    tok, width = tokens.shape[1], tokens.shape[2]
    half = width // 2
    slots = 16 * LINE * CAP
    lanes = LINE * tok
    ffe = gate_weight.shape[3]
    sds = jax.ShapeDtypeStruct
    anywhere = pl.BlockSpec(memory_space=HBM)

    swap = lambda v: shift(v, "section", 1, 2)
    ids = jnp.swapaxes(expert_ids[0], 1, 2)
    wts = jnp.swapaxes(route_weights[0], 1, 2)
    mine, start = pl.pallas_call(
        pack_kernel,
        out_shape=(sds((56, 128), F32), sds((tok, width), BF)),
        in_specs=[smem()] + [anywhere] * 5,
        out_specs=(vmem(), vmem()),
        scratch_shapes=[
            pltpu.VMEM((1, width), F32),
            pltpu.VMEM((1, 128), jnp.int32),
            pltpu.VMEM((2, 8, tok), jnp.int32),
            pltpu.VMEM((2, 8, tok), F32),
            pltpu.SemaphoreType.DMA((5,)),
        ],
        compiler_params=params(8),
        name="pack",
    )(section, *(pltpu.with_memory_space_constraint(v, HBM) for v in (tokens, norm_gain, expert_place, ids, wts)))
    theirs = swap(mine)

    low, high = pl.pallas_call(
        prepare_kernel,
        out_shape=(sds((tok, half), BF), sds((tok, half + 128), BF)),
        in_specs=[smem()] + [vmem()] * 3,
        out_specs=(vmem(), vmem()),
        compiler_params=params(16),
        name="prepare",
    )(section, start, mine, theirs)

    def experts(rows, layer, mats, mats_b):
        return pl.pallas_call(
            functools.partial(ffn_kernel, layer),
            out_shape=sds((slots, width), BF),
            in_specs=[smem(), vmem()] + [anywhere] * 3 + [pl.BlockSpec(memory_space=pl.ANY)] * 3,
            out_specs=vmem(),
            scratch_shapes=[
                pltpu.VMEM((width, ffe), BF),
                pltpu.VMEM((width, ffe), BF),
                pltpu.VMEM((ffe, width), BF),
                pltpu.VMEM((slots, ffe), F32),
                pltpu.VMEM((slots, ffe), F32),
                pltpu.VMEM((slots, ffe), BF),
                pltpu.SemaphoreType.DMA((5,)),
            ],
            compiler_params=params(32),
            name="experts",
        )(section, rows, *mats, *mats_b)

    def combine(rows, meta, layer):
        return pl.pallas_call(
            functools.partial(combine_kernel, layer),
            out_shape=[sds((tok, half), BF)] * (2 * LINE),
            in_specs=[smem(), vmem(), vmem()],
            out_specs=[vmem()] * (2 * LINE),
            compiler_params=params(20),
            name="combine",
        )(plane, meta, rows)

    def stagger(rows, layer):
        return pl.pallas_call(
            functools.partial(stagger_kernel, layer),
            out_shape=sds((slots, width), BF),
            in_specs=[smem(), vmem()],
            out_specs=vmem(),
            input_output_aliases={1: 0},
            compiler_params=params(8),
            name="stagger",
        )(section, rows)

    gather_scratch = [pltpu.VMEM((lanes, width), BF)]
    lows, highs = line_gather(low, high)
    outgoing, meta = pl.pallas_call(
        gather_first_kernel,
        out_shape=(sds((slots, width), BF), sds((lanes, 128), BF)),
        in_specs=[smem()] + [vmem()] * (2 * LINE),
        out_specs=(vmem(), vmem()),
        scratch_shapes=gather_scratch,
        compiler_params=params(20),
        name="spread",
    )(plane, *lows, *highs)

    mats = (gate_weight[0, 0], up_weight[0, 0], down_weight[0, 0])
    outgoing, mats = lax.optimization_barrier((outgoing, mats))
    mats_b = tuple(swap(m) for m in mats)
    mats = tuple(pltpu.with_memory_space_constraint(m, HBM) for m in mats)
    arrived = plane_exchange(stagger(outgoing, 0))
    returned = plane_exchange(experts(arrived, 0, mats, mats_b))
    sums = line_scatter(combine(returned, meta, 0))

    hidden, low, high = pl.pallas_call(
        middle_kernel,
        out_shape=(sds((tok, width), BF), sds((tok, half), BF), sds((tok, half), BF)),
        in_specs=[smem()] + [vmem()] * 9,
        out_specs=(vmem(), vmem(), vmem()),
        compiler_params=params(16),
        name="middle",
    )(section, start, mine, theirs, *sums)

    lows, highs = line_gather(low, high)
    outgoing = pl.pallas_call(
        gather_later_kernel,
        out_shape=sds((slots, width), BF),
        in_specs=[smem()] + [vmem()] * (2 * LINE + 1),
        out_specs=vmem(),
        scratch_shapes=gather_scratch,
        compiler_params=params(20),
        name="spread_later",
    )(plane, meta, *lows, *highs)
    returned = plane_exchange(experts(plane_exchange(stagger(outgoing, 1)), 1, mats, mats_b))
    sums = line_scatter(combine(returned, meta, 1))

    final = pl.pallas_call(
        last_kernel,
        out_shape=sds((tok, width), BF),
        in_specs=[vmem()] * 7,
        out_specs=vmem(),
        compiler_params=params(16),
        name="last",
    )(hidden, *sums)
    theirs = swap(final)
    mine_first = section[0] == 0
    return jnp.stack([jnp.where(mine_first, final, theirs), jnp.where(mine_first, theirs, final)])


def solution(mesh):
    fine = Mesh(mesh.devices.reshape(2, 4, 8, 4), ("section", "x", "z", "y"))
    line = ("x", "z", "y")
    in_specs = (
        P(None, line, None),
        P("section", None),
        P("section", line, None, None),
        P("section", line, None, None),
        P("section", line, None, None),
        P("section", None),
        P("section", None, line, None),
        P("section", None, line, None),
    )
    return jax.shard_map(
        local, mesh=fine, in_specs=in_specs, out_specs=P(None, line, None), check_vma=False
    )
```

```python
import functools

import jax
import jax.numpy as jnp
from jax import lax
from jax.experimental import pallas as pl
from jax.experimental.pallas import tpu as pltpu
from jax.sharding import Mesh, PartitionSpec as P

EPSILON = 1e-06
LINE = 8
CAP = 5
BF = jnp.bfloat16
F32 = jnp.float32
VMEM = pltpu.MemorySpace.VMEM
SMEM = pltpu.MemorySpace.SMEM
HBM = pltpu.MemorySpace.HBM


def vmem():
    return pl.BlockSpec(memory_space=VMEM)


def smem():
    return pl.BlockSpec(memory_space=SMEM)


def params(mib):
    return pltpu.CompilerParams(vmem_limit_bytes=mib << 20)


def shift(array, axis, by, size):
    return lax.ppermute(array, axis, [(i, (i + by) % size) for i in range(size)])


def normalized(hidden, gain):
    inverse = lax.rsqrt(jnp.mean(hidden * hidden, axis=-1, keepdims=True) + EPSILON)
    return (hidden * inverse * gain).astype(BF)


def routing_rows(ids, weights, place_row):
    tok = ids.shape[1]
    experts = lax.broadcasted_iota(jnp.int32, (128, tok), 0).astype(F32)
    hits = [(ids[k : k + 1, :] == experts).astype(F32) for k in range(8)]
    has = functools.reduce(jnp.add, hits)
    earlier = (
        lax.broadcasted_iota(jnp.int32, (tok, tok), 0) < lax.broadcasted_iota(jnp.int32, (tok, tok), 1)
    ).astype(F32)
    dot = functools.partial(jnp.dot, preferred_element_type=F32)
    before = dot(has.astype(BF), earlier.astype(BF))
    places = jnp.broadcast_to(place_row, (8, 128)).astype(BF)
    holders = [dot(places, h.astype(BF))[:1] for h in hits]
    positions = [jnp.sum(h * before, axis=0, keepdims=True) for h in hits]
    return jnp.concatenate(holders + positions + [weights, jnp.zeros_like(weights)], axis=0)


def pack_kernel(sec, tok, gain, place, ids, wts, table, hidden, gain_v, place_v, ids_v, wts_v, sems):
    copies = [
        pltpu.make_async_copy(gain, gain_v, sems.at[0]),
        pltpu.make_async_copy(place, place_v, sems.at[1]),
        pltpu.make_async_copy(ids, ids_v, sems.at[2]),
        pltpu.make_async_copy(wts, wts_v, sems.at[3]),
        pltpu.make_async_copy(tok.at[sec[0]], hidden, sems.at[4]),
    ]
    for c in copies:
        c.start()
    table[...] = jnp.zeros(table.shape, F32)
    for c in copies[:4]:
        c.wait()
    for i in range(16):
        table[i : i + 1, :] = gain_v[:, 128 * i : 128 * (i + 1)]
    for m in range(2):
        table[16 + 8 * m : 24 + 8 * m, :64] = ids_v[m].astype(F32)
        table[32 + 8 * m : 40 + 8 * m, :64] = wts_v[m]
    table[48:49, :] = place_v[...].astype(F32)
    copies[4].wait()


def gain_of(table):
    return jnp.concatenate([table[i : i + 1, :] for i in range(16)], axis=1)


def prepare_kernel(sec, hidden, mine, theirs, low, high):
    s = sec[0]
    first = jnp.where(s == 0, mine[...], theirs[...])
    second = jnp.where(s == 0, theirs[...], mine[...])
    half = hidden.shape[1] // 2
    normed = normalized(hidden[...].astype(F32), gain_of(first))
    low[...] = normed[:, :half]
    high[:, :half] = normed[:, half:]
    rows = []
    for table in (first, second):
        ids = jnp.where(s == 0, table[16:24, :64], table[24:32, :64])
        wts = jnp.where(s == 0, table[32:40, :64], table[40:48, :64])
        rows.append(routing_rows(ids, wts, table[48:49, :]))
    table = jnp.concatenate(rows, axis=0)
    table = jnp.concatenate([table, jnp.zeros_like(table)], axis=1)
    table = jnp.concatenate([table, jnp.zeros_like(table)], axis=0)
    high[:, half:] = table.T[: hidden.shape[0], :].astype(BF)


def gather_body(zi, metas, blocks_low, blocks_high, layer, out, whole, emit):
    tok = 64
    half = whole.shape[1] // 2
    for i in range(LINE):
        whole[i * tok : (i + 1) * tok, :half] = blocks_low[i][...]
        whole[i * tok : (i + 1) * tok, half:] = blocks_high[i][:, :half]
    meta = metas()
    if emit is not None:
        emit[...] = meta
    rows = meta.astype(F32).T[layer * 32 : layer * 32 + 16, :]
    holder = rows[:8].astype(jnp.int32)
    rank = rows[8:].astype(jnp.int32)
    block = lax.broadcasted_iota(jnp.int32, holder.shape, 1) // tok
    place = ((holder // 32) * 4 + holder % 4) * (LINE * CAP) + block * CAP + rank
    slot = jnp.where((holder // 4) % LINE == zi, place, -1)
    total = out.shape[0]
    lanes = LINE * tok
    step = 128
    for r in range(0, total, step):
        index = lax.broadcasted_iota(jnp.int32, (step, lanes), 0) + r
        hit = index == slot[0:1, :]
        for k in range(1, 8):
            hit = jnp.logical_or(hit, index == slot[k : k + 1, :])
        pick = jnp.where(hit, 1.0, 0.0).astype(BF)
        out[r : r + step, :] = jnp.dot(pick, whole[...], preferred_element_type=F32).astype(BF)


def gather_first_kernel(zi, *refs):
    low, high = refs[:LINE], refs[LINE : 2 * LINE]
    out, emit, whole = refs[2 * LINE :]
    half = low[0].shape[1]
    metas = lambda: jnp.concatenate([h[:, half:] for h in high], axis=0)
    gather_body(zi[0], metas, low, high, 0, out, whole, emit)


def gather_later_kernel(zi, meta, *refs):
    low, high = refs[:LINE], refs[LINE : 2 * LINE]
    out, whole = refs[2 * LINE :]
    gather_body(zi[0], lambda: meta[...], low, high, 1, out, whole, None)


def ffn_kernel(layer, sec, rows, ga, ua, da, gb, ub, db, out, wg, wu, wd, gate, up, hidden, sems):
    own = sec[0] == layer
    half = wg.shape[0] // 2
    pieces = []
    for a, b, dst, lo, size in (
        (ga, gb, wg, 0, half),
        (ua, ub, wu, 0, half),
        (ga, gb, wg, half, half),
        (ua, ub, wu, half, half),
        (da, db, wd, 0, wd.shape[0]),
    ):
        part = pl.ds(lo, size)
        n = len(pieces)
        pieces.append(
            (
                pltpu.make_async_copy(a.at[part], dst.at[part], sems.at[n]),
                pltpu.make_async_copy(b.at[part], dst.at[part], sems.at[n]),
            )
        )

    @pl.when(own)
    def _():
        for mine, _ in pieces:
            mine.start()

    @pl.when(jnp.logical_not(own))
    def _():
        for _, theirs in pieces:
            theirs.start()

    dot = functools.partial(jnp.dot, preferred_element_type=F32)
    pieces[0][0].wait()
    gate[...] = dot(rows[:, :half], wg[:half])
    pieces[1][0].wait()
    up[...] = dot(rows[:, :half], wu[:half])
    pieces[2][0].wait()
    pieces[3][0].wait()
    step = rows.shape[0] // 2
    for r in range(0, rows.shape[0], step):
        part = slice(r, r + step)
        v = gate[part] + dot(rows[part, half:], wg[half:])
        u = up[part] + dot(rows[part, half:], wu[half:])
        hidden[part] = (v / (1.0 + jnp.exp(-v)) * u).astype(BF)
    pieces[4][0].wait()
    for r in range(0, rows.shape[0], step):
        part = slice(r, r + step)
        out[part] = dot(hidden[part], wd[...]).astype(BF)


def combine_kernel(layer, zi, meta, rows, *outs):
    tok = 64
    half = rows.shape[1] // 2
    table = meta[:, layer * 32 : layer * 32 + 24].astype(F32)
    holder = table[:, :8].astype(jnp.int32)
    rank = table[:, 8:16].astype(jnp.int32)
    block = lax.broadcasted_iota(jnp.int32, holder.shape, 0) // tok
    place = ((holder // 32) * 4 + holder % 4) * (LINE * CAP) + block * CAP + rank
    slot = jnp.where((holder // 4) % LINE == zi[0], place, -1)
    total = rows.shape[0]
    for i in range(0, LINE, 2):
        part = slice(i * tok, (i + 2) * tok)
        index = lax.broadcasted_iota(jnp.int32, (2 * tok, total), 1)
        mix = jnp.zeros((2 * tok, total), F32)
        for k in range(8):
            mix = jnp.where(index == slot[part, k : k + 1], table[part, 16 + k : 17 + k], mix)
        mix = mix.astype(BF)
        for c in range(2):
            columns = slice(c * half, (c + 1) * half)
            sums = jnp.dot(mix, rows[:, columns], preferred_element_type=F32).astype(BF)
            at = i * tok
            base = 0
            for o in outs:
                size = o.shape[0]
                if at <= base < at + 2 * tok:
                    o[:, columns] = sums[base - at : base - at + size]
                base += size


def with_sums(hidden, sums):
    return (hidden[...].astype(F32) + sum(x[...].astype(F32) for x in sums)).astype(BF)


def middle_kernel(sec, start, mine, theirs, f, b, p, kept, low, high):
    hidden = with_sums(start, (p, f, b))
    kept[...] = hidden
    gain = gain_of(jnp.where(sec[0] == 0, theirs[:16, :], mine[:16, :]))
    normed = normalized(hidden.astype(F32), gain)
    half = low.shape[1]
    low[...] = normed[:, :half]
    high[...] = normed[:, half:]


def merge_kernel(top, came, own, far, out):
    tok = own.shape[0]
    half = tok // 2
    with_far = slice(0, half) if top else slice(half, tok)
    without = slice(half, tok) if top else slice(0, half)
    wide = lambda ref, rows: ref[rows, :].astype(F32)
    out[with_far, :] = (wide(came, with_far) + wide(own, with_far) + far[...].astype(F32)).astype(BF)
    out[without, :] = (wide(came, without) + wide(own, without)).astype(BF)


STAGGER = (13000, 10000)


def stagger_kernel(layer, sec, rows, out):
    @pl.when(sec[0] == layer)
    def _():
        pl.delay(STAGGER[layer])


def last_kernel(hidden, f, b, p, out):
    out[...] = with_sums(hidden, (p, f, b))


ORDER = (0, -1, 1, -2, 2, -3, 3, 4)


def line_gather(low, high):
    held = {0: (low, high)}
    ahead, behind = (low, high), (low, high)
    for step in (1, 2, 3):
        behind = tuple(shift(p, "z", 1, LINE) for p in behind)
        ahead = tuple(shift(p, "z", -1, LINE) for p in ahead)
        held[-step], held[step] = behind, ahead
    held[4] = (shift(behind[0], "z", 1, LINE), shift(ahead[1], "z", -1, LINE))
    return [held[o][0] for o in ORDER], [held[o][1] for o in ORDER]


def merge(top, came, own, far):
    return pl.pallas_call(
        functools.partial(merge_kernel, top),
        out_shape=jax.ShapeDtypeStruct(own.shape, BF),
        in_specs=[vmem()] * 3,
        out_specs=vmem(),
        compiler_params=params(4),
        name="merge",
    )(came, own, far)


def line_scatter(parts):
    own, b1, a1, b2, a2, b3, a3, top, bottom = parts
    up = lambda p, by=1: shift(p, "z", by, LINE)
    f, b = up(a3), up(b3, -1)
    top, bottom = up(top, 2), up(bottom, -2)
    f, b = up(merge(True, f, a2, top)), up(merge(False, b, b2, bottom), -1)
    return up(a1 + f), up(b1 + b, -1), own


def plane_exchange(rows):
    parts = rows.reshape(16, rows.shape[0] // 16, rows.shape[1])
    return lax.all_to_all(parts, ("x", "y"), 0, 0, tiled=True).reshape(rows.shape)


def local(
    tokens, norm_gain, gate_weight, up_weight, down_weight, expert_place, expert_ids, route_weights
):
    section = lax.axis_index("section").astype(jnp.int32)[None]
    plane = lax.axis_index("z").astype(jnp.int32)[None]
    tok, width = tokens.shape[1], tokens.shape[2]
    half = width // 2
    slots = 16 * LINE * CAP
    lanes = LINE * tok
    ffe = gate_weight.shape[3]
    sds = jax.ShapeDtypeStruct
    anywhere = pl.BlockSpec(memory_space=HBM)

    swap = lambda v: shift(v, "section", 1, 2)
    ids = jnp.swapaxes(expert_ids[0], 1, 2)
    wts = jnp.swapaxes(route_weights[0], 1, 2)
    mine, start = pl.pallas_call(
        pack_kernel,
        out_shape=(sds((56, 128), F32), sds((tok, width), BF)),
        in_specs=[smem()] + [anywhere] * 5,
        out_specs=(vmem(), vmem()),
        scratch_shapes=[
            pltpu.VMEM((1, width), F32),
            pltpu.VMEM((1, 128), jnp.int32),
            pltpu.VMEM((2, 8, tok), jnp.int32),
            pltpu.VMEM((2, 8, tok), F32),
            pltpu.SemaphoreType.DMA((5,)),
        ],
        compiler_params=params(8),
        name="pack",
    )(section, *(pltpu.with_memory_space_constraint(v, HBM) for v in (tokens, norm_gain, expert_place, ids, wts)))
    theirs = swap(mine)

    low, high = pl.pallas_call(
        prepare_kernel,
        out_shape=(sds((tok, half), BF), sds((tok, half + 128), BF)),
        in_specs=[smem()] + [vmem()] * 3,
        out_specs=(vmem(), vmem()),
        compiler_params=params(16),
        name="prepare",
    )(section, start, mine, theirs)

    def experts(rows, layer, mats, mats_b):
        return pl.pallas_call(
            functools.partial(ffn_kernel, layer),
            out_shape=sds((slots, width), BF),
            in_specs=[smem(), vmem()] + [anywhere] * 3 + [pl.BlockSpec(memory_space=pl.ANY)] * 3,
            out_specs=vmem(),
            scratch_shapes=[
                pltpu.VMEM((width, ffe), BF),
                pltpu.VMEM((width, ffe), BF),
                pltpu.VMEM((ffe, width), BF),
                pltpu.VMEM((slots, ffe), F32),
                pltpu.VMEM((slots, ffe), F32),
                pltpu.VMEM((slots, ffe), BF),
                pltpu.SemaphoreType.DMA((5,)),
            ],
            compiler_params=params(32),
            name="experts",
        )(section, rows, *mats, *mats_b)

    def combine(rows, meta, layer):
        return pl.pallas_call(
            functools.partial(combine_kernel, layer),
            out_shape=[sds((tok, width), BF)] * (LINE - 1) + [sds((tok // 2, width), BF)] * 2,
            in_specs=[smem(), vmem(), vmem()],
            out_specs=[vmem()] * (LINE + 1),
            compiler_params=params(20),
            name="combine",
        )(plane, meta, rows)

    def stagger(rows, layer):
        return pl.pallas_call(
            functools.partial(stagger_kernel, layer),
            out_shape=sds((slots, width), BF),
            in_specs=[smem(), vmem()],
            out_specs=vmem(),
            input_output_aliases={1: 0},
            compiler_params=params(8),
            name="stagger",
        )(section, rows)

    gather_scratch = [pltpu.VMEM((lanes, width), BF)]
    lows, highs = line_gather(low, high)
    outgoing, meta = pl.pallas_call(
        gather_first_kernel,
        out_shape=(sds((slots, width), BF), sds((lanes, 128), BF)),
        in_specs=[smem()] + [vmem()] * (2 * LINE),
        out_specs=(vmem(), vmem()),
        scratch_shapes=gather_scratch,
        compiler_params=params(20),
        name="spread",
    )(plane, *lows, *highs)

    mats = (gate_weight[0, 0], up_weight[0, 0], down_weight[0, 0])
    outgoing, mats = lax.optimization_barrier((outgoing, mats))
    mats_b = tuple(swap(m) for m in mats)
    mats = tuple(pltpu.with_memory_space_constraint(m, HBM) for m in mats)
    arrived = plane_exchange(stagger(outgoing, 0))
    returned = plane_exchange(experts(arrived, 0, mats, mats_b))
    sums = line_scatter(combine(returned, meta, 0))

    hidden, low, high = pl.pallas_call(
        middle_kernel,
        out_shape=(sds((tok, width), BF), sds((tok, half), BF), sds((tok, half), BF)),
        in_specs=[smem()] + [vmem()] * 6,
        out_specs=(vmem(), vmem(), vmem()),
        compiler_params=params(16),
        name="middle",
    )(section, start, mine, theirs, *sums)

    lows, highs = line_gather(low, high)
    outgoing = pl.pallas_call(
        gather_later_kernel,
        out_shape=sds((slots, width), BF),
        in_specs=[smem()] + [vmem()] * (2 * LINE + 1),
        out_specs=vmem(),
        scratch_shapes=gather_scratch,
        compiler_params=params(20),
        name="spread_later",
    )(plane, meta, *lows, *highs)
    returned = plane_exchange(experts(plane_exchange(stagger(outgoing, 1)), 1, mats, mats_b))
    sums = line_scatter(combine(returned, meta, 1))

    final = pl.pallas_call(
        last_kernel,
        out_shape=sds((tok, width), BF),
        in_specs=[vmem()] * 4,
        out_specs=vmem(),
        compiler_params=params(16),
        name="last",
    )(hidden, *sums)
    theirs = swap(final)
    mine_first = section[0] == 0
    return jnp.stack([jnp.where(mine_first, final, theirs), jnp.where(mine_first, theirs, final)])


def solution(mesh):
    fine = Mesh(mesh.devices.reshape(2, 4, 8, 4), ("section", "x", "z", "y"))
    line = ("x", "z", "y")
    in_specs = (
        P(None, line, None),
        P("section", None),
        P("section", line, None, None),
        P("section", line, None, None),
        P("section", line, None, None),
        P("section", None),
        P("section", None, line, None),
        P("section", None, line, None),
    )
    return jax.shard_map(
        local, mesh=fine, in_specs=in_specs, out_specs=P(None, line, None), check_vma=False
    )
```
